32 devices in a mesh: dp: 8 (over y, x, core), tensor: 4 (over z).
Axes of the slice: x: 2, y: 2, z: 4, core: 2. Of those that a mesh axis runs over, the one named last changes fastest.
Arguments:
- tokens: bfloat16 [512, 8192], P('dp'), may hold values from -6 to 6
- gate_weight: bfloat16 [8192, 14848], P('dp', 'tensor'), may hold values from -0.09375 to 0.09375
- up_weight: bfloat16 [8192, 14848], P('dp', 'tensor'), may hold values from -0.09375 to 0.09375
- down_weight: bfloat16 [14848, 8192], P('tensor', 'dp'), may hold values from -6 to 6
- channel_group: int32 [14848], P('tensor'), may hold values from 0 to 115, as said below
- owners: int32 [116], replicated, may hold values from 0 to 3
Outputs:
- group_scores: float32 [4, 116], P('tensor')
The draws below stay inside these ranges and needn't reach their ends.
Inputs may be any that keep to these rules, and one draw needn't show every extreme that they name: `channel_group`: every group 0 to 115 has exactly 128 channels.
All inputs are finite; a program needn't handle non-finite values.
Results may differ from the reference program's by a relative error of at most 0.0044.
Values may be sent and summed in bfloat16 or wider, within the bound.
A program may use at most 128 MiB of HBM per device.

```python
import jax
import jax.numpy as jnp
from jax import lax

D = 8192
FF = 14848
GROUP = 128
TOKENS = 512
GROUPS = 116
N_DP = 8
N_TENSOR = 4


def draw_channel_group(key, part):
    order = jax.random.permutation(jax.random.fold_in(key, 7), FF)
    return (order // GROUP).astype(jnp.int32)


def with_ends(result, own_key, low, high):
    extent = result.shape
    index_at = [jax.random.randint(jax.random.fold_in(own_key, axis), (), 0, extent[axis]) for axis in range(len(extent))]
    result = result.at[tuple(index_at)].set(low)
    longest = extent.index(max(extent))
    index_at[longest] = (index_at[longest] + 1) % extent[longest]
    return result.at[tuple(index_at)].set(high)


def spiked(drawn, own_key, source, target, blocks, factor):
    def block_of(position):
        return (jnp.arange(drawn.shape[position]) // (drawn.shape[position] // blocks)).reshape((-1,) + (1,) * (drawn.ndim - 1 - position))

    near = jax.random.permutation(own_key, blocks)[block_of(target)]
    second = (block_of(target) + blocks // 2) % blocks
    return jnp.where((block_of(source) == near) | (block_of(source) == second), factor * drawn, drawn)


def block_scale(stream_key, extent, shards, low, largest):
    level, own = 1.0, jax.random.fold_in(stream_key, 6)
    for position, blocks in shards:
        draws = jnp.exp(jax.random.uniform(jax.random.fold_in(own, position), (blocks,), jnp.float32, low / len(shards), largest / len(shards)))
        level = level * jnp.repeat(draws, extent[position] // blocks).reshape([-1 if axis == position else 1 for axis in range(len(extent))])
    return level


def noise(own_key, extent, spread, most, split=(), kind=jnp.bfloat16):
    result = jax.random.normal(own_key, extent, jnp.float32) * spread
    if len(split) > 0:
        result = block_scale(own_key, extent, split, -0.22, 0.18) * result
    return jnp.clip(result, min=-most, max=most).astype(kind)


def heavy_noise(stream_key, shape, spread, bound, cuts, heavy, held_as=jnp.bfloat16):
    entries = spread * jax.random.normal(stream_key, shape, jnp.float32)
    if cuts:
        entries = entries * block_scale(stream_key, shape, cuts, -0.22, 0.18)
    return jnp.clip(spiked(entries, jax.random.fold_in(stream_key, 3), *heavy), -bound, bound).astype(held_as)


def setup_inputs(seed: int = 0) -> dict:
    key_of = jax.random.split(jax.random.key(seed), 7)
    return {
        "tokens": noise(key_of[0], (TOKENS, D), 1.0, 6.0, ((0, 8),)),
        "gate_weight": heavy_noise(key_of[1], (D, FF), D ** -0.5, 0.09375, ((0, 8), (1, 4)), (0, 1, 8, 2.0)),
        "up_weight": heavy_noise(key_of[2], (D, FF), D ** -0.5, 0.09375, ((0, 8), (1, 4)), (0, 1, 8, 2.0)),
        "down_weight": heavy_noise(key_of[3], (FF, D), 1.0, 6.0, ((0, 4), (1, 8)), (1, 0, 8, 2.0)),
        "channel_group": draw_channel_group(jax.random.fold_in(key_of[6], 71), 0),
        "owners": with_ends(jax.random.randint(key_of[5], (GROUPS,), 0, N_TENSOR), jax.random.fold_in(key_of[5], 1), 0, N_TENSOR - 1).astype(jnp.int32),
    }


def reference(tokens, gate_weight, up_weight, down_weight, channel_group, owners):
    block = D // N_DP
    x_blocks = tokens.reshape(TOKENS, N_DP, block).transpose(1, 0, 2)
    g_blocks = gate_weight.reshape(N_DP, block, FF)
    u_blocks = up_weight.reshape(N_DP, block, FF)

    def add_block(carry, item):
        x_part, g_part, u_part = item
        pg = jnp.dot(x_part, g_part, preferred_element_type=jnp.float32).astype(jnp.bfloat16)
        pu = jnp.dot(x_part, u_part, preferred_element_type=jnp.float32).astype(jnp.bfloat16)
        pg, pu = lax.optimization_barrier((pg, pu))
        return ((carry[0] + pg.astype(jnp.float32), carry[1] + pu.astype(jnp.float32)), None)
    start = jnp.zeros((TOKENS, FF), jnp.float32)
    (gate, up), _ = lax.scan(add_block, (start, start), (x_blocks, g_blocks, u_blocks))
    hidden = jax.nn.silu(gate) * up
    energy = lax.optimization_barrier(jnp.sum(hidden * hidden, axis=0)) / TOKENS
    magnitude = lax.optimization_barrier(jnp.sum(jnp.abs(down_weight.astype(jnp.float32)), axis=1)) / D
    channel_score = jnp.sqrt(energy) * magnitude
    onehot = (channel_group[:, None] == jnp.arange(GROUPS, dtype=jnp.int32)[None, :]).astype(jnp.float32)
    totals = jnp.dot(channel_score, onehot, precision=lax.Precision.HIGHEST) / GROUP
    ranks = jnp.arange(N_TENSOR, dtype=jnp.int32)[:, None]
    return jnp.where(owners[None, :] == ranks, totals[None, :], jnp.float32(0.0))
```

```python
import functools

import jax
import jax.numpy as jnp
from jax import lax
from jax.experimental import pallas as pl
from jax.experimental.pallas import tpu as pltpu
from jax.sharding import PartitionSpec as P

GROUP = 128
LANES = 128
ROLES = 4
LAG_CORE = 2
LAG_FIRST = 7
LAG_SECOND = 3
MESH = pl.DeviceIdType.MESH


def group_sum(channel_score, groups, count):
    onehot = (groups[:, None] == jnp.arange(count, dtype=jnp.int32)[None, :]).astype(jnp.float32)
    return jnp.dot(channel_score, onehot, precision=lax.Precision.HIGHEST) / GROUP


def plain_shards(tokens, gate_weight, up_weight, down_weight, channel_group, owners):
    total_tokens = tokens.shape[0] * lax.axis_size("dp")
    width = gate_weight.shape[1]
    group_count = owners.shape[0]
    magnitude = jnp.sum(jnp.abs(down_weight.astype(jnp.float32)), axis=1) / tokens.shape[1]
    columns = lax.all_to_all(tokens, "dp", split_axis=1, concat_axis=0, tiled=True)
    mixed = lax.psum_scatter(
        jnp.concatenate(
            (
                jnp.dot(columns, gate_weight, preferred_element_type=jnp.float32),
                jnp.dot(columns, up_weight, preferred_element_type=jnp.float32),
            ),
            axis=1,
        ).astype(jnp.bfloat16),
        "dp",
        scatter_dimension=0,
        tiled=True,
    ).astype(jnp.float32)
    hidden = jax.nn.silu(mixed[:, :width]) * mixed[:, width:]
    energy = jnp.sum(hidden * hidden, axis=0) / total_tokens
    energy, magnitude = lax.psum((energy, magnitude), "dp")
    partial_value = group_sum(jnp.sqrt(energy) * magnitude, channel_group, group_count)
    totals = lax.psum(partial_value, "tensor")
    rank = lax.axis_index("tensor")
    row = jnp.where(owners == rank, totals, jnp.float32(0.0))
    return row[None, :]


def kernel(
    n_tensor,
    tok_ref,
    gate_ref,
    up_ref,
    down_ref,
    group_ref,
    owner_ref,
    out_ref,
    tok_buf,
    x_buf,
    w_buf,
    d_buf,
    group_buf,
    owner_buf,
    give,
    keep,
    got_core,
    got_first,
    got_second,
    give_x,
    keep_x,
    got_core_x,
    got_first_x,
    got_second_x,
    energy,
    shared,
    mag_out,
    magnitude,
    score,
    totals,
    local_sem,
    g_sem,
    u_sem,
    d_sem,
    x_send,
    x_recv,
    core_send,
    core_recv,
    first_send,
    first_recv,
    second_send,
    second_recv,
    core_x_send,
    core_x_recv,
    first_x_send,
    first_x_recv,
    second_x_send,
    second_x_recv,
    m_send,
    m_recv,
    s_send,
    s_recv,
    e_send,
    e_recv,
    t_send,
    t_recv,
    seen,
):
    n_dp = 8
    chunks = w_buf.shape[0]
    quads, extra = chunks // ROLES, chunks % ROLES
    items = 4 * quads
    block = tok_ref.shape[0]
    depth = x_buf.shape[2]
    me = lax.axis_index("dp")
    z = lax.axis_index("tensor")
    c, x, y = me % 2, (me // 2) % 2, me // 4
    chip = me // 2

    def chip_at(f, s):
        fx, fy = f * (1 - c) + s * c, f * c + s * (1 - c)
        return 2 * (y + fy * (1 - 2 * y)) + x + fx * (1 - 2 * x)

    def device_at(f, s, same):
        return 2 * chip_at(f, s) + (c if same else 1 - c)

    core_peer = device_at(0, 0, False)
    first_peer = device_at(1, 0, True)
    second_peer = device_at(0, 1, True)
    others = [(r % 2, r // 2, same) for r in range(4) for same in (False, True) if (r, same) != (0, True)]

    def remote(src, dst, send, recv, peer, plane=z):
        return pltpu.make_async_remote_copy(
            src_ref=src, dst_ref=dst, send_sem=send, recv_sem=recv, device_id=(peer, plane), device_id_type=MESH
        )

    barrier = pltpu.get_barrier_semaphore()
    near = [hop for hop in others if hop[0] + hop[1] < 2]
    for hop in near:
        pl.semaphore_signal(barrier, inc=1, device_id=(device_at(*hop), z), device_id_type=MESH)

    def signal_planes(sem):
        @pl.when(z > 0)
        def _():
            pl.semaphore_signal(sem, inc=1, device_id=(me, z - 1), device_id_type=MESH)

        @pl.when(z < n_tensor - 1)
        def _():
            pl.semaphore_signal(sem, inc=1, device_id=(me, z + 1), device_id_type=MESH)

    planes = jnp.where(z > 0, 1, 0) + jnp.where(z < n_tensor - 1, 1, 0)
    signal_planes(barrier)

    load_tokens = pltpu.make_async_copy(tok_ref, tok_buf, local_sem.at[0])
    load_groups = pltpu.make_async_copy(group_ref, group_buf, local_sem.at[1])
    load_owners = pltpu.make_async_copy(owner_ref, owner_buf, local_sem.at[2])
    load_tokens.start()

    def gate_copy(i):
        cols = pl.ds(pl.multiple_of(i * LANES, LANES), LANES)
        return pltpu.make_async_copy(gate_ref.at[:, cols], w_buf.at[i, :, pl.ds(0, LANES)], g_sem.at[i])

    def up_copy(i):
        cols = pl.ds(pl.multiple_of(i * LANES, LANES), LANES)
        return pltpu.make_async_copy(up_ref.at[:, cols], w_buf.at[i, :, pl.ds(LANES, LANES)], u_sem.at[i])

    def down_copy(i):
        rows = pl.ds(pl.multiple_of(i * LANES, LANES), LANES)
        return pltpu.make_async_copy(down_ref.at[rows, :], d_buf.at[i], d_sem.at[i])

    for i in list(range(ROLES)) + list(range(chunks - extra, chunks)):
        gate_copy(i).start()
        up_copy(i).start()

    @pl.loop(ROLES, chunks - extra)
    def _(i):
        gate_copy(i).start()
        up_copy(i).start()

    def token_copy(r, same):
        peer = device_at(r % 2, r // 2, same)
        cols = pl.ds(pl.multiple_of(peer * depth, depth), depth)
        slot = 2 * r + (1 if same else 0)
        rows = pl.ds(block if same else 0, block)
        return remote(tok_buf.at[:, cols], x_buf.at[r, rows, :], x_send.at[slot], x_recv.at[slot], peer)

    load_tokens.wait()
    pl.semaphore_wait(barrier, len(near) + planes)
    token_copy(0, False).start()
    for same in (True, False):
        token_copy(1, same).start()
    load_groups.start()
    load_owners.start()

    @pl.loop(0, chunks)
    def _(i):
        down_copy(i).start()

    own_cols = pl.ds(pl.multiple_of(me * depth, depth), depth)
    x_buf[0, block:, :] = tok_buf[:, own_cols]
    mag_out[...] = jnp.zeros_like(mag_out)
    energy[...] = jnp.zeros_like(energy)
    shared[...] = jnp.zeros_like(shared)
    ones = jnp.ones((8, d_buf.shape[2]), jnp.bfloat16)

    def other_row(j, step):
        r = j // quads
        return j + quads * (step - 2 * step * ((r // step) % 2))

    def core_copy(j):
        return remote(give.at[j], got_core.at[j], core_send.at[j], core_recv.at[j], core_peer)

    def first_copy(j, to):
        return remote(keep.at[j, pl.ds(2, 2)], got_first.at[to], first_send.at[j], first_recv.at[to], first_peer)

    def second_copy(j, to):
        return remote(keep.at[j, 1], got_second.at[to], second_send.at[j], second_recv.at[to], second_peer)

    def core_x_copy(r, e):
        j = r * extra + e
        return remote(give_x.at[j], got_core_x.at[j], core_x_send.at[j], core_x_recv.at[j], core_peer)

    def first_x_copy(half, e):
        j = half * extra + e
        source = (2 * half + 1) * extra + e
        return remote(keep_x.at[source], got_first_x.at[j], first_x_send.at[j], first_x_recv.at[j], first_peer)

    def second_x_copy(e):
        return remote(
            keep_x.at[2 * extra + e], got_second_x.at[e], second_x_send.at[e], second_x_recv.at[e], second_peer
        )

    def share_copy(n):
        return remote(shared.at[me], shared.at[me], s_send.at[n], s_recv.at[n], device_at(*others[n]))

    def magnitude_copy(n):
        f, s, same = others[n]
        return remote(mag_out.at[chip_at(f, s)], magnitude.at[me], m_send.at[n], m_recv.at[n], device_at(f, s, same))

    def total(*refs):
        value = refs[0].astype(jnp.float32)
        for ref in refs[1:]:
            value = value + ref.astype(jnp.float32)
        return value

    def squares(mixed):
        gate, up = mixed[:, :LANES], mixed[:, LANES:]
        hidden = gate / (1.0 + jnp.exp(-gate)) * up
        return jnp.sum(hidden * hidden, axis=0, keepdims=True)

    swap = (0, 2, 1, 3)
    magnitude_start = quads + 1
    magnitude_end = magnitude_start + -(-chunks // 2)
    last_fold = 3 * quads + LAG_FIRST
    steps = last_fold + LAG_SECOND + quads
    rounds = [(quads + 2) + 4 * n for n in range(n_tensor - 1)]

    token_copy(0, False).wait_recv()

    def step(it, on):
        after_core = it - LAG_CORE
        after_first = it - LAG_FIRST
        final = it - last_fold - LAG_SECOND
        r = it // quads
        core_row = after_core // quads
        for k in range(1, 4):

            @pl.when(it == k * quads)
            def _():
                token_copy(k, False).wait_recv()
                token_copy(k, True).wait_recv()

        @pl.when(it == 2)
        def _():
            for same in (True, False):
                token_copy(2, same).start()

        @pl.when(it == quads)
        def _():
            for same in (True, False):
                token_copy(3, same).start()

        for n, at in enumerate(rounds):

            @pl.when(it == at)
            def _():
                if n > 0:
                    pl.semaphore_wait(seen.at[n - 1], planes)
                signal_planes(seen.at[n])

        @pl.when((after_core >= 0) & (after_core < items))
        def _():
            core_copy(after_core).wait_recv()
            keep[after_core, 2:] = total(keep[after_core, 2:], got_core[after_core, 2:]).astype(jnp.bfloat16)

        if extra:

            @pl.when((after_core >= 0) & (after_core < items) & (after_core % quads == 0))
            def _():
                for e in range(extra):
                    core_x_copy(core_row, e).wait_recv()
                    j = core_row * extra + e
                    keep_x[j] = jnp.where(
                        core_row % 2 == 1, total(keep_x[j], got_core_x[j]), keep_x[j].astype(jnp.float32)
                    ).astype(jnp.bfloat16)

        @pl.when(it < items)
        def _():
            u = it % quads

            @pl.when(r == 0)
            def _():
                for k in range(ROLES):
                    gate_copy(ROLES * u + k).wait()
                    up_copy(ROLES * u + k).wait()

            for role in (2, 3, 1, 0):
                product = jnp.dot(
                    x_buf[r], w_buf[ROLES * u + chip_at(role // 2, role % 2)], preferred_element_type=jnp.float32
                ).astype(jnp.bfloat16)
                give[it, swap[role]] = product[:block]
                keep[it, role] = product[block:]

        if extra:

            @pl.when((it < items) & (it % quads == 0))
            def _():
                for e in range(extra):

                    @pl.when(r == 0)
                    def _():
                        gate_copy(chunks - extra + e).wait()
                        up_copy(chunks - extra + e).wait()

                    product = jnp.dot(
                        x_buf[r], w_buf[chunks - extra + e], preferred_element_type=jnp.float32
                    ).astype(jnp.bfloat16)
                    give_x[r * extra + e] = product[:block]
                    keep_x[r * extra + e] = product[block:]

        @pl.when((after_core >= 0) & (after_core < items))
        def _():
            first_copy(after_core, other_row(after_core, 1)).start()

        if extra:

            @pl.when((after_core >= 0) & (after_core < items) & (after_core % quads == 0) & (core_row % 2 == 1))
            def _():
                for e in range(extra):
                    first_x_copy(core_row // 2, e).start()

        @pl.when(it < items)
        def _():
            core_copy(it).start()

        if extra:

            @pl.when((it < items) & (it % quads == 0))
            def _():
                for e in range(extra):
                    core_x_copy(r, e).start()

        folding = ((after_first >= quads) & (after_first < 2 * quads)) | (
            (after_first >= 3 * quads) & (after_first < items)
        )

        @pl.when(folding)
        def _():
            for j in (after_first - quads, after_first):
                first_copy(j, j).wait_recv()
                keep[j, 1] = total(keep[j, 1], got_core[j, 1], got_first[j, 1]).astype(jnp.bfloat16)

        if extra:

            @pl.when(after_first == 3 * quads)
            def _():
                for e in range(extra):
                    first_x_copy(1, e).wait_recv()
                    j = 2 * extra + e
                    keep_x[j] = total(keep_x[j], got_core_x[j], got_first_x[extra + e]).astype(jnp.bfloat16)

        @pl.when((it >= magnitude_start) & (it < magnitude_end))
        def _():
            for k in range(2):
                i = 2 * (it - magnitude_start) + k

                @pl.when(i < chunks)
                def _():
                    down_copy(i).wait()
                    sums = lax.dot_general(
                        ones, jnp.abs(d_buf[i]), (((1,), (1,)), ((), ())), preferred_element_type=jnp.float32
                    )[0:1, :]

                    @pl.when(i < items)
                    def _():
                        mag_out[i % ROLES, pl.ds(i // ROLES, 1), :] = sums

                    @pl.when(i >= items)
                    def _():
                        for k in range(ROLES):
                            mag_out[k, pl.ds(quads + i - items, 1), :] = sums

        @pl.when(it == magnitude_end)
        def _():
            for n in range(n_dp - 1):
                magnitude_copy(n).start()
            magnitude[me] = mag_out[chip]

        @pl.when(folding)
        def _():
            for j in (after_first - quads, after_first):
                second_copy(j, other_row(j, 2)).start()

        if extra:

            @pl.when(after_first == 3 * quads)
            def _():
                for e in range(extra):
                    second_x_copy(e).start()

            @pl.when(final == 0)
            def _():
                for e in range(extra):
                    first_x_copy(0, e).wait_recv()
                    second_x_copy(e).wait_recv()
                    shared[me, e : e + 1, :] = squares(
                        total(keep_x[e], got_core_x[e], got_first_x[e], got_second_x[e])
                    )

        @pl.when(final >= 0)
        def _():
            value = jnp.zeros((1, LANES), jnp.float32)
            for k in range(4):
                j = k * quads + final
                second_copy(j, j).wait_recv()
                value = value + squares(total(keep[j, 0], got_core[j, 0], got_first[j, 0], got_second[j]))
            energy[c, pl.ds(final, 1), :] = value

        if extra:

            @pl.when(final == 0)
            def _():
                for n in range(n_dp - 1):
                    share_copy(n).start()

        return on

    lax.fori_loop(0, steps, step, 0)

    energy_copy = remote(energy.at[c], energy.at[c], e_send, e_recv, core_peer)
    energy_copy.start()
    load_groups.wait()
    load_owners.wait()
    for n in range(n_dp - 1):
        magnitude_copy(n).wait_recv()
        if extra:
            share_copy(n).wait_recv()
    mag = magnitude[0]
    for k in range(1, n_dp):
        mag = mag + magnitude[k]
    mag = mag / tok_ref.shape[1]
    if n_tensor > 1:
        pl.semaphore_wait(seen.at[n_tensor - 2], planes)
    tokens = block * n_dp
    if extra:
        both = shared[0]
        for k in range(1, n_dp):
            both = both + shared[k]
        shares = jnp.sqrt(both[:extra] / tokens) * mag[quads : quads + extra]
        shares = jnp.where(chip == 0, shares, 0.0)
    energy_copy.wait()
    score[...] = jnp.sqrt((energy[0] + energy[1]) / tokens) * mag

    lines = lax.broadcasted_iota(jnp.int32, (totals.shape[2], LANES), 0)
    acc = jnp.zeros(lines.shape, jnp.float32)
    for u in range(quads):
        acc = acc + jnp.where(lines == group_buf[pl.ds(ROLES * u + chip, 1), :], score[u : u + 1, :], 0.0)
    for e in range(extra):
        acc = acc + jnp.where(lines == group_buf[items + e : items + e + 1, :], shares[e : e + 1], 0.0)
    slot = ROLES * z + chip
    totals[slot] = jnp.sum(acc.T, axis=0, keepdims=True)
    t_copies = []
    for dz in range(n_tensor):
        for k in range(4):
            if dz or k:
                n = len(t_copies)
                copy = remote(
                    totals.at[slot],
                    totals.at[slot],
                    t_send.at[n],
                    t_recv.at[n],
                    device_at(k % 2, k // 2, True),
                    (z + dz) % n_tensor,
                )
                copy.start()
                t_copies.append(copy)

    for r in range(4):
        for same in (False, True):
            if (r, same) != (0, True):
                token_copy(r, same).wait_send()
    for n in range(n_dp - 1):
        magnitude_copy(n).wait_send()
        if extra:
            share_copy(n).wait_send()

    @pl.loop(0, items)
    def _(j):
        core_copy(j).wait_send()
        first_copy(j, j).wait_send()
        second_copy(j, j).wait_send()

    for e in range(extra):
        for r in range(4):
            core_x_copy(r, e).wait_send()
        for half in range(2):
            first_x_copy(half, e).wait_send()
        second_x_copy(e).wait_send()

    for copy in t_copies:
        copy.wait()
    row = totals[0]
    for k in range(1, ROLES * n_tensor):
        row = row + totals[k]
    row = row[:, : out_ref.shape[1]] / GROUP
    out_ref[...] = jnp.where(owner_buf[...] == z, row, 0.0)


def fused_shards(n_dp, n_tensor, tokens, gate_weight, up_weight, down_weight, channel_group, owners):
    block = tokens.shape[0]
    depth, width = gate_weight.shape
    chunks = width // LANES
    quads, extra = chunks // ROLES, chunks % ROLES
    items, spare = 4 * quads, max(extra, 1)
    count = owners.shape[0]
    span = down_weight.shape[1]
    lines = -(-(quads + extra) // 8) * 8
    padded = -(-count // LANES) * LANES
    peers = n_dp - 1
    far = max(4 * n_tensor - 1, 1)
    vmem = pl.BlockSpec(memory_space=pltpu.VMEM)
    hbm = pl.BlockSpec(memory_space=pl.ANY)
    dma = pltpu.SemaphoreType.DMA
    tile = (block, 2 * LANES)
    half = jnp.bfloat16
    return pl.pallas_call(
        functools.partial(kernel, n_tensor),
        out_shape=jax.ShapeDtypeStruct((1, count), jnp.float32),
        in_specs=[hbm, hbm, hbm, hbm, hbm, hbm],
        out_specs=vmem,
        scratch_shapes=[
            pltpu.VMEM(tokens.shape, half),
            pltpu.VMEM((4, 2 * block, depth), half),
            pltpu.VMEM((chunks, depth, 2 * LANES), half),
            pltpu.VMEM((chunks, LANES, span), half),
            pltpu.VMEM((chunks, LANES), jnp.int32),
            pltpu.VMEM((1, count), jnp.int32),
            pltpu.VMEM((items, ROLES) + tile, half),
            pltpu.VMEM((items, ROLES) + tile, half),
            pltpu.VMEM((items, ROLES) + tile, half),
            pltpu.VMEM((items, 2) + tile, half),
            pltpu.VMEM((items,) + tile, half),
            pltpu.VMEM((4 * spare,) + tile, half),
            pltpu.VMEM((4 * spare,) + tile, half),
            pltpu.VMEM((4 * spare,) + tile, half),
            pltpu.VMEM((2 * spare,) + tile, half),
            pltpu.VMEM((spare,) + tile, half),
            pltpu.VMEM((2, lines, LANES), jnp.float32),
            pltpu.VMEM((n_dp, 8, LANES), jnp.float32),
            pltpu.VMEM((ROLES, lines, LANES), jnp.float32),
            pltpu.VMEM((n_dp, lines, LANES), jnp.float32),
            pltpu.VMEM((lines, LANES), jnp.float32),
            pltpu.VMEM((ROLES * n_tensor, 1, padded), jnp.float32),
            dma((3,)),
            dma((chunks,)),
            dma((chunks,)),
            dma((chunks,)),
            dma((n_dp,)),
            dma((n_dp,)),
            dma((items,)),
            dma((items,)),
            dma((items,)),
            dma((items,)),
            dma((items,)),
            dma((items,)),
            dma((4 * spare,)),
            dma((4 * spare,)),
            dma((2 * spare,)),
            dma((2 * spare,)),
            dma((spare,)),
            dma((spare,)),
            dma((peers,)),
            dma((peers,)),
            dma((peers,)),
            dma((peers,)),
            dma,
            dma,
            dma((far,)),
            dma((far,)),
            pltpu.SemaphoreType.REGULAR((max(n_tensor - 1, 1),)),
        ],
        compiler_params=pltpu.CompilerParams(
            collective_id=0, has_side_effects=True, vmem_limit_bytes=56 * 1024 * 1024
        ),
    )(tokens, gate_weight, up_weight, down_weight, channel_group.reshape(chunks, LANES), owners.reshape(1, count))


def solution(mesh):
    n_dp, n_tensor = mesh.shape["dp"], mesh.shape["tensor"]

    def shards(tokens, gate_weight, *rest):
        if n_dp == 8 and gate_weight.shape[1] % LANES == 0 and gate_weight.shape[1] >= ROLES * LANES:
            return fused_shards(n_dp, n_tensor, tokens, gate_weight, *rest)
        return plain_shards(tokens, gate_weight, *rest)

    return jax.shard_map(
        shards,
        mesh=mesh,
        in_specs=(
            P("dp", None),
            P("dp", "tensor"),
            P("dp", "tensor"),
            P("tensor", "dp"),
            P("tensor"),
            P(),
        ),
        out_specs=P("tensor", None),
        check_vma=False,
    )
```

```python
import functools

import jax
import jax.numpy as jnp
from jax import lax
from jax.experimental import pallas as pl
from jax.experimental.pallas import tpu as pltpu
from jax.sharding import PartitionSpec as P

GROUP = 128
LANES = 128
ROLES = 4
LAG_CORE = 2
LAG_FIRST = 7
HOLD = 0
LAG_SECOND = 3
MAGNITUDES = 3
MAGNITUDE_ROW = 2
SPLIT = (2, 3)
SHARE_SECOND = 4
SHARE_LAST = 5
MESH = pl.DeviceIdType.MESH


def group_sum(channel_score, groups, count):
    onehot = (groups[:, None] == jnp.arange(count, dtype=jnp.int32)[None, :]).astype(jnp.float32)
    return jnp.dot(channel_score, onehot, precision=lax.Precision.HIGHEST) / GROUP


def plain_shards(tokens, gate_weight, up_weight, down_weight, channel_group, owners):
    total_tokens = tokens.shape[0] * lax.axis_size("dp")
    width = gate_weight.shape[1]
    group_count = owners.shape[0]
    magnitude = jnp.sum(jnp.abs(down_weight.astype(jnp.float32)), axis=1) / tokens.shape[1]
    columns = lax.all_to_all(tokens, "dp", split_axis=1, concat_axis=0, tiled=True)
    mixed = lax.psum_scatter(
        jnp.concatenate(
            (
                jnp.dot(columns, gate_weight, preferred_element_type=jnp.float32),
                jnp.dot(columns, up_weight, preferred_element_type=jnp.float32),
            ),
            axis=1,
        ).astype(jnp.bfloat16),
        "dp",
        scatter_dimension=0,
        tiled=True,
    ).astype(jnp.float32)
    hidden = jax.nn.silu(mixed[:, :width]) * mixed[:, width:]
    energy = jnp.sum(hidden * hidden, axis=0) / total_tokens
    energy, magnitude = lax.psum((energy, magnitude), "dp")
    partial_value = group_sum(jnp.sqrt(energy) * magnitude, channel_group, group_count)
    totals = lax.psum(partial_value, "tensor")
    rank = lax.axis_index("tensor")
    row = jnp.where(owners == rank, totals, jnp.float32(0.0))
    return row[None, :]


def kernel(
    n_tensor,
    tok_ref,
    gate_ref,
    up_ref,
    down_ref,
    group_ref,
    owner_ref,
    out_ref,
    tok_buf,
    x_buf,
    w_buf,
    d_buf,
    group_buf,
    owner_buf,
    give,
    keep,
    got_core,
    got_first,
    got_second,
    give_x,
    keep_x,
    got_core_x,
    got_first_x,
    got_second_x,
    energy,
    shared,
    mag_out,
    magnitude,
    score,
    totals,
    local_sem,
    g_sem,
    u_sem,
    d_sem,
    x_send,
    x_recv,
    core_send,
    core_recv,
    first_send,
    first_recv,
    second_send,
    second_recv,
    core_x_send,
    core_x_recv,
    first_x_send,
    first_x_recv,
    second_x_send,
    second_x_recv,
    m_send,
    m_recv,
    s_send,
    s_recv,
    e_send,
    e_recv,
    t_send,
    t_recv,
    z_send,
    z_recv,
    seen,
    met,
):
    n_dp = 8
    chunks = w_buf.shape[0]
    quads, extra = chunks // ROLES, chunks % ROLES
    items = 4 * quads
    block = tok_ref.shape[0]
    depth = x_buf.shape[2]
    me = lax.axis_index("dp")
    z = lax.axis_index("tensor")
    c, x, y = me % 2, (me // 2) % 2, me // 4
    chip = me // 2

    def chip_at(f, s):
        fx, fy = f * (1 - c) + s * c, f * c + s * (1 - c)
        return 2 * (y + fy * (1 - 2 * y)) + x + fx * (1 - 2 * x)

    def device_at(f, s, same):
        return 2 * chip_at(f, s) + (c if same else 1 - c)

    core_peer = device_at(0, 0, False)
    first_peer = device_at(1, 0, True)
    second_peer = device_at(0, 1, True)
    others = [(r % 2, r // 2, same) for r in range(4) for same in (False, True) if (r, same) != (0, True)]

    def remote(src, dst, send, recv, peer, plane=z):
        return pltpu.make_async_remote_copy(
            src_ref=src, dst_ref=dst, send_sem=send, recv_sem=recv, device_id=(peer, plane), device_id_type=MESH
        )

    barrier = pltpu.get_barrier_semaphore()
    near = [hop for hop in others if hop[0] + hop[1] < 2]
    for hop in near:
        pl.semaphore_signal(barrier, inc=1, device_id=(device_at(*hop), z), device_id_type=MESH)

    def signal_planes(sem):
        @pl.when(z > 0)
        def _():
            pl.semaphore_signal(sem, inc=1, device_id=(me, z - 1), device_id_type=MESH)

        @pl.when(z < n_tensor - 1)
        def _():
            pl.semaphore_signal(sem, inc=1, device_id=(me, z + 1), device_id_type=MESH)

    planes = jnp.where(z > 0, 1, 0) + jnp.where(z < n_tensor - 1, 1, 0)
    signal_planes(barrier)

    load_tokens = pltpu.make_async_copy(tok_ref, tok_buf, local_sem.at[0])
    load_groups = pltpu.make_async_copy(group_ref, group_buf, local_sem.at[1])
    load_owners = pltpu.make_async_copy(owner_ref, owner_buf, local_sem.at[2])
    load_tokens.start()

    def gate_copy(i):
        cols = pl.ds(pl.multiple_of(i * LANES, LANES), LANES)
        return pltpu.make_async_copy(gate_ref.at[:, cols], w_buf.at[i, :, pl.ds(0, LANES)], g_sem.at[i])

    def up_copy(i):
        cols = pl.ds(pl.multiple_of(i * LANES, LANES), LANES)
        return pltpu.make_async_copy(up_ref.at[:, cols], w_buf.at[i, :, pl.ds(LANES, LANES)], u_sem.at[i])

    def down_copy(i):
        rows = pl.ds(pl.multiple_of(i * LANES, LANES), LANES)
        return pltpu.make_async_copy(down_ref.at[rows, :], d_buf.at[i], d_sem.at[i])

    for i in list(range(ROLES)) + list(range(chunks - extra, chunks)):
        gate_copy(i).start()
        up_copy(i).start()

    @pl.loop(ROLES, chunks - extra)
    def _(i):
        gate_copy(i).start()
        up_copy(i).start()

    piece = block // n_tensor

    def split(r):
        return r in SPLIT and n_tensor > 1 and block % (16 * n_tensor) == 0

    def token_copy(r, same):
        peer = device_at(r % 2, r // 2, same)
        cols = pl.ds(pl.multiple_of(peer * depth, depth), depth)
        slot = 2 * r + (1 if same else 0)
        start = block if same else 0
        if split(r):
            source = pl.ds(pl.multiple_of(z * piece, piece), piece)
            rows = pl.ds(pl.multiple_of(start + z * piece, piece), piece)
        else:
            source, rows = pl.ds(0, block), pl.ds(start, block)
        return remote(tok_buf.at[source, cols], x_buf.at[r, rows, :], x_send.at[slot], x_recv.at[slot], peer)

    def plane_copies(r):
        copies = []
        for same in (False, True):
            rows = pl.ds(pl.multiple_of((block if same else 0) + z * piece, piece), piece)
            for dz in range(1, n_tensor):
                n = (2 * r + (1 if same else 0)) * n_tensor + dz
                data = x_buf.at[r, rows, :]
                copies.append(remote(data, data, z_send.at[n], z_recv.at[n], me, (z + dz) % n_tensor))
        return copies

    load_tokens.wait()
    pl.semaphore_wait(barrier, len(near) + planes)
    token_copy(0, False).start()
    for same in (True, False):
        token_copy(1, same).start()
    for same in (True, False):
        token_copy(2, same).start()
    if n_tensor > 2:
        signal_planes(met.at[0])
    load_groups.start()
    load_owners.start()

    @pl.loop(0, chunks)
    def _(i):
        down_copy(i).start()

    own_cols = pl.ds(pl.multiple_of(me * depth, depth), depth)
    x_buf[0, block:, :] = tok_buf[:, own_cols]
    mag_out[...] = jnp.zeros_like(mag_out)
    energy[...] = jnp.zeros_like(energy)
    shared[...] = jnp.zeros_like(shared)
    ones = jnp.ones((8, d_buf.shape[2]), jnp.bfloat16)

    def other_row(j, step):
        r = j // quads
        return j + quads * (step - 2 * step * ((r // step) % 2))

    def core_copy(j):
        return remote(give.at[j], got_core.at[j], core_send.at[j], core_recv.at[j], core_peer)

    def first_copy(j, to):
        return remote(keep.at[j, pl.ds(2, 2)], got_first.at[to], first_send.at[j], first_recv.at[to], first_peer)

    def second_copy(j, to):
        return remote(keep.at[j, 1], got_second.at[to], second_send.at[j], second_recv.at[to], second_peer)

    def core_x_copy(r, e):
        j = r * extra + e
        return remote(give_x.at[j], got_core_x.at[j], core_x_send.at[j], core_x_recv.at[j], core_peer)

    def first_x_copy(half, e):
        j = half * extra + e
        source = (2 * half + 1) * extra + e
        return remote(keep_x.at[source], got_first_x.at[j], first_x_send.at[j], first_x_recv.at[j], first_peer)

    def second_x_copy(e):
        return remote(
            keep_x.at[2 * extra + e], got_second_x.at[e], second_x_send.at[e], second_x_recv.at[e], second_peer
        )

    def share_copy(n):
        return remote(shared.at[me], shared.at[me], s_send.at[n], s_recv.at[n], device_at(*others[n]))

    def magnitude_copy(n):
        f, s, same = others[n]
        return remote(mag_out.at[chip_at(f, s)], magnitude.at[me], m_send.at[n], m_recv.at[n], device_at(f, s, same))

    def total(*refs):
        value = refs[0].astype(jnp.float32)
        for ref in refs[1:]:
            value = value + ref.astype(jnp.float32)
        return value

    def squares(mixed):
        gate, up = mixed[:, :LANES], mixed[:, LANES:]
        hidden = gate / (1.0 + jnp.exp(-gate)) * up
        return jnp.sum(hidden * hidden, axis=0, keepdims=True)

    def fold(j):
        first_copy(j, j).wait_recv()
        keep[j, 1] = total(keep[j, 1], got_core[j, 1], got_first[j, 1]).astype(jnp.bfloat16)

    swap = (0, 2, 1, 3)
    magnitude_start = MAGNITUDE_ROW * quads
    magnitude_end = magnitude_start + -(-chunks // MAGNITUDES)
    last_fold = 3 * quads + LAG_FIRST
    steps = last_fold + LAG_SECOND + quads
    rounds = [(quads + 2) + 4 * n for n in range(n_tensor - 1)]

    token_copy(0, False).wait_recv()

    def step(it, on):
        after_core = it - LAG_CORE
        after_first = it - LAG_FIRST
        final = it - last_fold - LAG_SECOND
        r = it // quads
        core_row = after_core // quads
        @pl.when(it == quads)
        def _():
            for same in (True, False):
                token_copy(1, same).wait_recv()
            for same in (True, False):
                token_copy(3, same).start()

        for n in range(n_tensor - 2):

            @pl.when(it == 1 + n)
            def _():
                pl.semaphore_wait(met.at[n], planes)
                if n < n_tensor - 3:
                    signal_planes(met.at[n + 1])

        for k, at in ((2, min(SHARE_SECOND, 2 * quads)), (3, min(quads + SHARE_LAST, 3 * quads))):
            if split(k):

                @pl.when(it == at)
                def _():
                    for same in (True, False):
                        token_copy(k, same).wait_recv()
                    for copy in plane_copies(k):
                        copy.start()

        for k in (2, 3):

            @pl.when(it == k * quads)
            def _():
                for copy in plane_copies(k) if split(k) else [token_copy(k, same) for same in (True, False)]:
                    copy.wait_recv()

        for n, at in enumerate(rounds):

            @pl.when(it == at)
            def _():
                if n > 0:
                    pl.semaphore_wait(seen.at[n - 1], planes)
                signal_planes(seen.at[n])

        @pl.when((after_core >= 0) & (after_core < items))
        def _():
            core_copy(after_core).wait_recv()
            keep[after_core, 2:] = total(keep[after_core, 2:], got_core[after_core, 2:]).astype(jnp.bfloat16)

        if extra:

            @pl.when((after_core >= 0) & (after_core < items) & (after_core % quads == 0))
            def _():
                for e in range(extra):
                    core_x_copy(core_row, e).wait_recv()
                    j = core_row * extra + e
                    keep_x[j] = jnp.where(
                        core_row % 2 == 1, total(keep_x[j], got_core_x[j]), keep_x[j].astype(jnp.float32)
                    ).astype(jnp.bfloat16)

        @pl.when(it < items)
        def _():
            u = it % quads

            @pl.when(r == 0)
            def _():
                for k in range(ROLES):
                    gate_copy(ROLES * u + k).wait()
                    up_copy(ROLES * u + k).wait()

            for role in (2, 3, 1, 0):
                product = jnp.dot(
                    x_buf[r], w_buf[ROLES * u + chip_at(role // 2, role % 2)], preferred_element_type=jnp.float32
                ).astype(jnp.bfloat16)
                give[it, swap[role]] = product[:block]
                keep[it, role] = product[block:]

        if extra:

            @pl.when((it < items) & (it % quads == 0))
            def _():
                for e in range(extra):

                    @pl.when(r == 0)
                    def _():
                        gate_copy(chunks - extra + e).wait()
                        up_copy(chunks - extra + e).wait()

                    product = jnp.dot(
                        x_buf[r], w_buf[chunks - extra + e], preferred_element_type=jnp.float32
                    ).astype(jnp.bfloat16)
                    give_x[r * extra + e] = product[:block]
                    keep_x[r * extra + e] = product[block:]

        @pl.when((after_core >= 0) & (after_core < items))
        def _():
            first_copy(after_core, other_row(after_core, 1)).start()

        if extra:

            @pl.when((after_core >= 0) & (after_core < items) & (after_core % quads == 0) & (core_row % 2 == 1))
            def _():
                for e in range(extra):
                    first_x_copy(core_row // 2, e).start()

        @pl.when(it < items)
        def _():
            core_copy(it).start()

        if extra:

            @pl.when((it < items) & (it % quads == 0))
            def _():
                for e in range(extra):
                    core_x_copy(r, e).start()

        early = after_first - HOLD
        folding = ((after_first >= 3 * quads) & (after_first < items), (early >= quads) & (early < 2 * quads))

        for on_fold, at in zip(folding, (after_first, early)):

            @pl.when(on_fold)
            def _():
                for j in (at - quads, at):
                    fold(j)

        if extra:

            @pl.when(after_first == 3 * quads)
            def _():
                for e in range(extra):
                    first_x_copy(1, e).wait_recv()
                    j = 2 * extra + e
                    keep_x[j] = total(keep_x[j], got_core_x[j], got_first_x[extra + e]).astype(jnp.bfloat16)

        @pl.when((it >= magnitude_start) & (it < magnitude_end))
        def _():
            for k in range(MAGNITUDES):
                i = MAGNITUDES * (it - magnitude_start) + k

                @pl.when(i < chunks)
                def _():
                    down_copy(i).wait()
                    sums = lax.dot_general(
                        ones, jnp.abs(d_buf[i]), (((1,), (1,)), ((), ())), preferred_element_type=jnp.float32
                    )[0:1, :]

                    @pl.when(i < items)
                    def _():
                        mag_out[i % ROLES, pl.ds(i // ROLES, 1), :] = sums

                    @pl.when(i >= items)
                    def _():
                        for k in range(ROLES):
                            mag_out[k, pl.ds(quads + i - items, 1), :] = sums

        @pl.when(it == magnitude_end)
        def _():
            for n in range(n_dp - 1):
                magnitude_copy(n).start()
            magnitude[me] = mag_out[chip]

        for on_fold, at in zip(folding, (after_first, early)):

            @pl.when(on_fold)
            def _():
                for j in (at - quads, at):
                    second_copy(j, other_row(j, 2)).start()

        if extra:

            @pl.when(after_first == 3 * quads)
            def _():
                for e in range(extra):
                    second_x_copy(e).start()

            @pl.when(final == 0)
            def _():
                for e in range(extra):
                    first_x_copy(0, e).wait_recv()
                    second_x_copy(e).wait_recv()
                    shared[me, e : e + 1, :] = squares(
                        total(keep_x[e], got_core_x[e], got_first_x[e], got_second_x[e])
                    )

        @pl.when(final >= 0)
        def _():
            value = jnp.zeros((1, LANES), jnp.float32)
            for k in range(4):
                j = k * quads + final
                second_copy(j, j).wait_recv()
                value = value + squares(total(keep[j, 0], got_core[j, 0], got_first[j, 0], got_second[j]))
            energy[c, pl.ds(final, 1), :] = value

        if extra:

            @pl.when(final == 0)
            def _():
                for n in range(n_dp - 1):
                    share_copy(n).start()

        return on

    lax.fori_loop(0, steps, step, 0)

    energy_copy = remote(energy.at[c], energy.at[c], e_send, e_recv, core_peer)
    energy_copy.start()
    load_groups.wait()
    load_owners.wait()
    for n in range(n_dp - 1):
        magnitude_copy(n).wait_recv()
        if extra:
            share_copy(n).wait_recv()
    mag = magnitude[0]
    for k in range(1, n_dp):
        mag = mag + magnitude[k]
    mag = mag / tok_ref.shape[1]
    if n_tensor > 1:
        pl.semaphore_wait(seen.at[n_tensor - 2], planes)
    tokens = block * n_dp
    if extra:
        both = shared[0]
        for k in range(1, n_dp):
            both = both + shared[k]
        shares = jnp.sqrt(both[:extra] / tokens) * mag[quads : quads + extra]
        shares = jnp.where(chip == 0, shares, 0.0)
    energy_copy.wait()
    score[...] = jnp.sqrt((energy[0] + energy[1]) / tokens) * mag

    lines = lax.broadcasted_iota(jnp.int32, (totals.shape[2], LANES), 0)
    acc = jnp.zeros(lines.shape, jnp.float32)
    for u in range(quads):
        acc = acc + jnp.where(lines == group_buf[pl.ds(ROLES * u + chip, 1), :], score[u : u + 1, :], 0.0)
    for e in range(extra):
        acc = acc + jnp.where(lines == group_buf[items + e : items + e + 1, :], shares[e : e + 1], 0.0)
    slot = ROLES * z + chip
    totals[slot] = jnp.sum(acc.T, axis=0, keepdims=True)
    t_copies = []
    for dz in range(n_tensor):
        for k in range(4):
            if dz or k:
                n = len(t_copies)
                copy = remote(
                    totals.at[slot],
                    totals.at[slot],
                    t_send.at[n],
                    t_recv.at[n],
                    device_at(k % 2, k // 2, True),
                    (z + dz) % n_tensor,
                )
                copy.start()
                t_copies.append(copy)

    for r in range(4):
        for same in (False, True):
            if (r, same) != (0, True):
                token_copy(r, same).wait_send()
        if split(r):
            for copy in plane_copies(r):
                copy.wait_send()
    for n in range(n_dp - 1):
        magnitude_copy(n).wait_send()
        if extra:
            share_copy(n).wait_send()

    @pl.loop(0, items)
    def _(j):
        core_copy(j).wait_send()
        first_copy(j, j).wait_send()
        second_copy(j, j).wait_send()

    for e in range(extra):
        for r in range(4):
            core_x_copy(r, e).wait_send()
        for half in range(2):
            first_x_copy(half, e).wait_send()
        second_x_copy(e).wait_send()

    for copy in t_copies:
        copy.wait()
    row = totals[0]
    for k in range(1, ROLES * n_tensor):
        row = row + totals[k]
    row = row[:, : out_ref.shape[1]] / GROUP
    out_ref[...] = jnp.where(owner_buf[...] == z, row, 0.0)


def fused_shards(n_dp, n_tensor, tokens, gate_weight, up_weight, down_weight, channel_group, owners):
    block = tokens.shape[0]
    depth, width = gate_weight.shape
    chunks = width // LANES
    quads, extra = chunks // ROLES, chunks % ROLES
    items, spare = 4 * quads, max(extra, 1)
    count = owners.shape[0]
    span = down_weight.shape[1]
    lines = -(-(quads + extra) // 8) * 8
    padded = -(-count // LANES) * LANES
    peers = n_dp - 1
    far = max(4 * n_tensor - 1, 1)
    vmem = pl.BlockSpec(memory_space=pltpu.VMEM)
    hbm = pl.BlockSpec(memory_space=pl.ANY)
    dma = pltpu.SemaphoreType.DMA
    tile = (block, 2 * LANES)
    half = jnp.bfloat16
    return pl.pallas_call(
        functools.partial(kernel, n_tensor),
        out_shape=jax.ShapeDtypeStruct((1, count), jnp.float32),
        in_specs=[hbm, hbm, hbm, hbm, hbm, hbm],
        out_specs=vmem,
        scratch_shapes=[
            pltpu.VMEM(tokens.shape, half),
            pltpu.VMEM((4, 2 * block, depth), half),
            pltpu.VMEM((chunks, depth, 2 * LANES), half),
            pltpu.VMEM((chunks, LANES, span), half),
            pltpu.VMEM((chunks, LANES), jnp.int32),
            pltpu.VMEM((1, count), jnp.int32),
            pltpu.VMEM((items, ROLES) + tile, half),
            pltpu.VMEM((items, ROLES) + tile, half),
            pltpu.VMEM((items, ROLES) + tile, half),
            pltpu.VMEM((items, 2) + tile, half),
            pltpu.VMEM((items,) + tile, half),
            pltpu.VMEM((4 * spare,) + tile, half),
            pltpu.VMEM((4 * spare,) + tile, half),
            pltpu.VMEM((4 * spare,) + tile, half),
            pltpu.VMEM((2 * spare,) + tile, half),
            pltpu.VMEM((spare,) + tile, half),
            pltpu.VMEM((2, lines, LANES), jnp.float32),
            pltpu.VMEM((n_dp, 8, LANES), jnp.float32),
            pltpu.VMEM((ROLES, lines, LANES), jnp.float32),
            pltpu.VMEM((n_dp, lines, LANES), jnp.float32),
            pltpu.VMEM((lines, LANES), jnp.float32),
            pltpu.VMEM((ROLES * n_tensor, 1, padded), jnp.float32),
            dma((3,)),
            dma((chunks,)),
            dma((chunks,)),
            dma((chunks,)),
            dma((n_dp,)),
            dma((n_dp,)),
            dma((items,)),
            dma((items,)),
            dma((items,)),
            dma((items,)),
            dma((items,)),
            dma((items,)),
            dma((4 * spare,)),
            dma((4 * spare,)),
            dma((2 * spare,)),
            dma((2 * spare,)),
            dma((spare,)),
            dma((spare,)),
            dma((peers,)),
            dma((peers,)),
            dma((peers,)),
            dma((peers,)),
            dma,
            dma,
            dma((far,)),
            dma((far,)),
            dma((n_dp * n_tensor,)),
            dma((n_dp * n_tensor,)),
            pltpu.SemaphoreType.REGULAR((max(n_tensor - 1, 1),)),
            pltpu.SemaphoreType.REGULAR((max(n_tensor - 2, 1),)),
        ],
        compiler_params=pltpu.CompilerParams(
            collective_id=0, has_side_effects=True, vmem_limit_bytes=56 * 1024 * 1024
        ),
    )(tokens, gate_weight, up_weight, down_weight, channel_group.reshape(chunks, LANES), owners.reshape(1, count))


def solution(mesh):
    n_dp, n_tensor = mesh.shape["dp"], mesh.shape["tensor"]

    def shards(tokens, gate_weight, *rest):
        if n_dp == 8 and gate_weight.shape[1] % LANES == 0 and gate_weight.shape[1] >= ROLES * LANES:
            return fused_shards(n_dp, n_tensor, tokens, gate_weight, *rest)
        return plain_shards(tokens, gate_weight, *rest)

    return jax.shard_map(
        shards,
        mesh=mesh,
        in_specs=(
            P("dp", None),
            P("dp", "tensor"),
            P("dp", "tensor"),
            P("tensor", "dp"),
            P("tensor"),
            P(),
        ),
        out_specs=P("tensor", None),
        check_vma=False,
    )
```

```python
import functools

import jax
import jax.numpy as jnp
from jax import lax
from jax.experimental import pallas as pl
from jax.experimental.pallas import tpu as pltpu
from jax.sharding import PartitionSpec as P

GROUP = 128
LANES = 128
ROLES = 4
LAG_CORE = 2
LAG_FIRST = 7
HOLD = 0
LAG_SECOND = 3
MAGNITUDE_ROW = 2
SPLIT = (2, 3)
SHARE_SECOND = 4
SHARE_LAST = 5
MESH = pl.DeviceIdType.MESH


def group_sum(channel_score, groups, count):
    onehot = (groups[:, None] == jnp.arange(count, dtype=jnp.int32)[None, :]).astype(jnp.float32)
    return jnp.dot(channel_score, onehot, precision=lax.Precision.HIGHEST) / GROUP


def plain_shards(tokens, gate_weight, up_weight, down_weight, channel_group, owners):
    total_tokens = tokens.shape[0] * lax.axis_size("dp")
    width = gate_weight.shape[1]
    group_count = owners.shape[0]
    magnitude = jnp.sum(jnp.abs(down_weight.astype(jnp.float32)), axis=1) / tokens.shape[1]
    columns = lax.all_to_all(tokens, "dp", split_axis=1, concat_axis=0, tiled=True)
    mixed = lax.psum_scatter(
        jnp.concatenate(
            (
                jnp.dot(columns, gate_weight, preferred_element_type=jnp.float32),
                jnp.dot(columns, up_weight, preferred_element_type=jnp.float32),
            ),
            axis=1,
        ).astype(jnp.bfloat16),
        "dp",
        scatter_dimension=0,
        tiled=True,
    ).astype(jnp.float32)
    hidden = jax.nn.silu(mixed[:, :width]) * mixed[:, width:]
    energy = jnp.sum(hidden * hidden, axis=0) / total_tokens
    energy, magnitude = lax.psum((energy, magnitude), "dp")
    partial_value = group_sum(jnp.sqrt(energy) * magnitude, channel_group, group_count)
    totals = lax.psum(partial_value, "tensor")
    rank = lax.axis_index("tensor")
    row = jnp.where(owners == rank, totals, jnp.float32(0.0))
    return row[None, :]


def kernel(
    n_tensor,
    tok_ref,
    gate_ref,
    up_ref,
    down_ref,
    group_ref,
    owner_ref,
    out_ref,
    tok_buf,
    x_buf,
    w_buf,
    d_buf,
    group_buf,
    owner_buf,
    give,
    keep,
    got_core,
    got_first,
    got_second,
    give_x,
    keep_x,
    got_core_x,
    got_first_x,
    got_second_x,
    energy,
    shared,
    mag_out,
    magnitude,
    score,
    totals,
    local_sem,
    tok_sem,
    g_sem,
    u_sem,
    d_sem,
    x_send,
    x_recv,
    core_send,
    core_recv,
    first_send,
    first_recv,
    second_send,
    second_recv,
    core_x_send,
    core_x_recv,
    first_x_send,
    first_x_recv,
    second_x_send,
    second_x_recv,
    m_send,
    m_recv,
    s_send,
    s_recv,
    e_send,
    e_recv,
    t_send,
    t_recv,
    z_send,
    z_recv,
    seen,
    met,
):
    n_dp = 8
    chunks = w_buf.shape[0]
    quads, extra = chunks // ROLES, chunks % ROLES
    items = 4 * quads
    block = tok_ref.shape[0]
    depth = x_buf.shape[2]
    me = lax.axis_index("dp")
    z = lax.axis_index("tensor")
    c, x, y = me % 2, (me // 2) % 2, me // 4
    chip = me // 2

    def chip_at(f, s):
        fx, fy = f * (1 - c) + s * c, f * c + s * (1 - c)
        return 2 * (y + fy * (1 - 2 * y)) + x + fx * (1 - 2 * x)

    def device_at(f, s, same):
        return 2 * chip_at(f, s) + (c if same else 1 - c)

    core_peer = device_at(0, 0, False)
    first_peer = device_at(1, 0, True)
    second_peer = device_at(0, 1, True)
    others = [(r % 2, r // 2, same) for r in range(4) for same in (False, True) if (r, same) != (0, True)]

    def remote(src, dst, send, recv, peer, plane=z):
        return pltpu.make_async_remote_copy(
            src_ref=src, dst_ref=dst, send_sem=send, recv_sem=recv, device_id=(peer, plane), device_id_type=MESH
        )

    barrier = pltpu.get_barrier_semaphore()
    near = [hop for hop in others if hop[0] + hop[1] < 2]
    for hop in near:
        pl.semaphore_signal(barrier, inc=1, device_id=(device_at(*hop), z), device_id_type=MESH)

    def signal_planes(sem):
        @pl.when(z > 0)
        def _():
            pl.semaphore_signal(sem, inc=1, device_id=(me, z - 1), device_id_type=MESH)

        @pl.when(z < n_tensor - 1)
        def _():
            pl.semaphore_signal(sem, inc=1, device_id=(me, z + 1), device_id_type=MESH)

    planes = jnp.where(z > 0, 1, 0) + jnp.where(z < n_tensor - 1, 1, 0)
    signal_planes(barrier)

    load_groups = pltpu.make_async_copy(group_ref, group_buf, local_sem.at[0])
    load_owners = pltpu.make_async_copy(owner_ref, owner_buf, local_sem.at[1])
    piece = block // n_tensor

    def split(r):
        return r in SPLIT and n_tensor > 1 and block % (16 * n_tensor) == 0

    def token_rows(r, start):
        if split(r):
            return pl.ds(pl.multiple_of(start + z * piece, piece), piece)
        return pl.ds(start, block)

    def token_columns(f, s, same):
        return pl.ds(pl.multiple_of(device_at(f, s, same) * depth, depth), depth)

    def token_load(n):
        f, s, same = others[n]
        data = (token_rows(f + 2 * s, 0), token_columns(f, s, same))
        return pltpu.make_async_copy(tok_ref.at[data], tok_buf.at[data], tok_sem.at[n])

    load_own = pltpu.make_async_copy(
        tok_ref.at[:, token_columns(0, 0, True)], x_buf.at[0, pl.ds(block, block), :], local_sem.at[2]
    )
    load_own.start()
    for n in range(3):
        token_load(n).start()

    def gate_copy(i):
        cols = pl.ds(pl.multiple_of(i * LANES, LANES), LANES)
        return pltpu.make_async_copy(gate_ref.at[:, cols], w_buf.at[i, :, pl.ds(0, LANES)], g_sem.at[i])

    def up_copy(i):
        cols = pl.ds(pl.multiple_of(i * LANES, LANES), LANES)
        return pltpu.make_async_copy(up_ref.at[:, cols], w_buf.at[i, :, pl.ds(LANES, LANES)], u_sem.at[i])

    def down_copy(i):
        rows = pl.ds(pl.multiple_of(i * LANES, LANES), LANES)
        return pltpu.make_async_copy(down_ref.at[rows, :], d_buf.at[i], d_sem.at[i])

    for i in range(ROLES):
        gate_copy(i).start()
        up_copy(i).start()
    for n in range(3, len(others)):
        token_load(n).start()

    @pl.loop(ROLES, chunks)
    def _(i):
        gate_copy(i).start()
        up_copy(i).start()

    def token_copy(r, same):
        cols = token_columns(r % 2, r // 2, same)
        slot = 2 * r + (1 if same else 0)
        start = block if same else 0
        return remote(
            tok_buf.at[token_rows(r, 0), cols],
            x_buf.at[r, token_rows(r, start), :],
            x_send.at[slot],
            x_recv.at[slot],
            device_at(r % 2, r // 2, same),
        )

    def plane_copies(r):
        copies = []
        for same in (False, True):
            data = x_buf.at[r, token_rows(r, block if same else 0), :]
            for dz in range(1, n_tensor):
                n = (2 * r + (1 if same else 0)) * n_tensor + dz
                copies.append(remote(data, data, z_send.at[n], z_recv.at[n], me, (z + dz) % n_tensor))
        return copies

    sends = [(f + 2 * s, same) for f, s, same in others]
    token_load(0).wait()
    pl.semaphore_wait(barrier, len(near) + planes)
    token_copy(*sends[0]).start()
    for n in range(1, 5):
        token_load(n).wait()
        token_copy(*sends[n]).start()
    if n_tensor > 2:
        signal_planes(met.at[0])
    load_groups.start()
    load_owners.start()

    @pl.loop(0, chunks)
    def _(i):
        down_copy(i).start()

    mag_out[...] = jnp.zeros_like(mag_out)
    energy[...] = jnp.zeros_like(energy)
    shared[...] = jnp.zeros_like(shared)
    ones = jnp.ones((8, d_buf.shape[2]), jnp.bfloat16)

    def core_copy(j):
        return remote(give.at[j], got_core.at[j], core_send.at[j], core_recv.at[j], core_peer)

    def first_copy(j, to):
        return remote(keep.at[j, pl.ds(2, 2)], got_first.at[to], first_send.at[j], first_recv.at[to], first_peer)

    def second_copy(j, to):
        return remote(keep.at[j, 1], got_second.at[to], second_send.at[j], second_recv.at[to], second_peer)

    def core_x_copy(r, e):
        j = r * extra + e
        return remote(give_x.at[j], got_core_x.at[j], core_x_send.at[j], core_x_recv.at[j], core_peer)

    def first_x_copy(half, e):
        j = half * extra + e
        source = (2 * half + 1) * extra + e
        return remote(keep_x.at[source], got_first_x.at[j], first_x_send.at[j], first_x_recv.at[j], first_peer)

    def second_x_copy(e):
        return remote(
            keep_x.at[2 * extra + e], got_second_x.at[e], second_x_send.at[e], second_x_recv.at[e], second_peer
        )

    def share_copy(n):
        return remote(shared.at[me], shared.at[me], s_send.at[n], s_recv.at[n], device_at(*others[n]))

    def magnitude_copy(n):
        f, s, same = others[n]
        return remote(mag_out.at[chip_at(f, s)], magnitude.at[me], m_send.at[n], m_recv.at[n], device_at(f, s, same))

    def total(*refs):
        value = refs[0].astype(jnp.float32)
        for ref in refs[1:]:
            value = value + ref.astype(jnp.float32)
        return value

    def squares(mixed):
        gate, up = mixed[:, :LANES], mixed[:, LANES:]
        hidden = gate / (1.0 + jnp.exp(-gate)) * up
        return jnp.sum(hidden * hidden, axis=0, keepdims=True)

    swap = (0, 2, 1, 3)
    role_chips = [chip_at(role // 2, role % 2) for role in range(ROLES)]

    def multiply(r, u, j):
        for role in (2, 3, 1, 0):
            product = jnp.dot(
                x_buf[r], w_buf[ROLES * u + role_chips[role]], preferred_element_type=jnp.float32
            ).astype(jnp.bfloat16)
            give[j, swap[role]] = product[:block]
            keep[j, role] = product[block:]

    def fold(j):
        first_copy(j, j).wait_recv()
        keep[j, 1] = total(keep[j, 1], got_core[j, 1], got_first[j, 1]).astype(jnp.bfloat16)

    def finish(j):
        second_copy(j, j).wait_recv()
        return squares(total(keep[j, 0], got_core[j, 0], got_first[j, 0], got_second[j]))

    fold_starts = (quads + LAG_FIRST + HOLD, 3 * quads + LAG_FIRST)
    final_start = fold_starts[1] + LAG_SECOND
    steps = final_start + quads
    magnitude_start = MAGNITUDE_ROW * quads

    def row_at(it, lag):
        return (it - lag) // quads if 0 <= it - lag < items else None

    def stages(it):
        return (
            row_at(it, 0),
            row_at(it, LAG_CORE),
            tuple(0 <= it - start < quads for start in fold_starts),
            0 <= it - magnitude_start < quads,
            0 <= it - final_start < quads,
        )

    def step(now, it):
        row, core_row, folding, weighing, ending = now
        after_core = it - LAG_CORE
        if core_row is not None:
            core_copy(after_core).wait_recv()
            keep[after_core, 2:] = total(keep[after_core, 2:], got_core[after_core, 2:]).astype(jnp.bfloat16)
        if row is not None:
            u = it - row * quads
            if row == 0:
                for k in range(ROLES):
                    gate_copy(ROLES * u + k).wait()
                    up_copy(ROLES * u + k).wait()
            multiply(row, u, it)
        if core_row is not None:
            first_copy(after_core, after_core + (-quads if core_row % 2 else quads)).start()
        if row is not None:
            core_copy(it).start()
        for half in range(2):
            if folding[half]:
                for r in (2 * half, 2 * half + 1):
                    fold(it - fold_starts[half] + r * quads)
        if weighing:
            v = it - magnitude_start
            for k in range(ROLES):
                down_copy(ROLES * v + k).wait()
            rows = jnp.abs(d_buf[pl.ds(ROLES * v, ROLES)].reshape(ROLES * LANES, d_buf.shape[2]))
            sums = lax.dot_general(ones, rows, (((1,), (1,)), ((), ())), preferred_element_type=jnp.float32)
            for k in range(ROLES):
                mag_out[k, pl.ds(v, 1), :] = sums[0:1, k * LANES : (k + 1) * LANES]
        for half in range(2):
            if folding[half]:
                for r in (2 * half, 2 * half + 1):
                    j = it - fold_starts[half] + r * quads
                    second_copy(j, j + (-2 * quads if half else 2 * quads)).start()
        if folding[1]:
            u = it - fold_starts[1]
            energy[c, pl.ds(u, 1), :] = finish(u + 2 * quads) + finish(u + 3 * quads)
        if ending:
            u = it - final_start
            energy[c, pl.ds(u, 1), :] = energy[c, pl.ds(u, 1), :] + (finish(u) + finish(u + quads))

    events = {}

    def at(it):
        return lambda run: events.setdefault(it, []).append(run)

    @at(quads)
    def _():
        for same in (True, False):
            token_copy(1, same).wait_recv()
        for n in range(5, 7):
            token_load(n).wait()
            token_copy(*sends[n]).start()

    for n in range(n_tensor - 2):

        @at(1 + n)
        def _(n=n):
            pl.semaphore_wait(met.at[n], planes)
            if n < n_tensor - 3:
                signal_planes(met.at[n + 1])

    for k, when in ((2, min(SHARE_SECOND, 2 * quads)), (3, min(quads + SHARE_LAST, 3 * quads))):
        if split(k):

            @at(when)
            def _(k=k):
                for same in (True, False):
                    token_copy(k, same).wait_recv()
                for copy in plane_copies(k):
                    copy.start()

    for k in (2, 3):

        @at(k * quads)
        def _(k=k):
            for copy in plane_copies(k) if split(k) else [token_copy(k, same) for same in (True, False)]:
                copy.wait_recv()

    for n in range(n_tensor - 1):

        @at(quads + 2 + 4 * n)
        def _(n=n):
            if n > 0:
                pl.semaphore_wait(seen.at[n - 1], planes)
            signal_planes(seen.at[n])

    for e in range(extra):
        for r in range(4):
            when = r * quads if r else min(4, quads - 1)

            @at(when)
            def _(r=r, e=e):
                if r == 0:
                    gate_copy(items + e).wait()
                    up_copy(items + e).wait()
                product = jnp.dot(x_buf[r], w_buf[items + e], preferred_element_type=jnp.float32).astype(jnp.bfloat16)
                give_x[r * extra + e] = product[:block]
                keep_x[r * extra + e] = product[block:]
                core_x_copy(r, e).start()

            @at(when + LAG_CORE)
            def _(r=r, e=e):
                core_x_copy(r, e).wait_recv()
                j = r * extra + e
                if r % 2:
                    keep_x[j] = total(keep_x[j], got_core_x[j]).astype(jnp.bfloat16)
                    first_x_copy(r // 2, e).start()

        @at(fold_starts[1])
        def _(e=e):
            first_x_copy(1, e).wait_recv()
            j = 2 * extra + e
            keep_x[j] = total(keep_x[j], got_core_x[j], got_first_x[extra + e]).astype(jnp.bfloat16)
            second_x_copy(e).start()

        @at(magnitude_start + quads)
        def _(e=e):
            down_copy(items + e).wait()
            sums = lax.dot_general(
                ones, jnp.abs(d_buf[items + e]), (((1,), (1,)), ((), ())), preferred_element_type=jnp.float32
            )
            for k in range(ROLES):
                mag_out[k, quads + e : quads + e + 1, :] = sums[0:1, :]

        @at(fold_starts[1] + quads - 1)
        def _(e=e):
            first_x_copy(0, e).wait_recv()
            second_x_copy(e).wait_recv()
            shared[me, e : e + 1, :] = squares(total(keep_x[e], got_core_x[e], got_first_x[e], got_second_x[e]))

    @at(magnitude_start + quads + 1)
    def _():
        for n in range(n_dp - 1):
            magnitude_copy(n).start()
        magnitude[me] = mag_out[chip]

    if extra:

        @at(fold_starts[1] + quads)
        def _():
            for n in range(n_dp - 1):
                share_copy(n).start()

    load_own.wait()
    token_copy(0, False).wait_recv()
    low = 0
    while low < steps:
        for run in events.pop(low, ()):
            run()
        now, high = stages(low), low + 1
        while high < steps and stages(high) == now and high not in events:
            high += 1
        if high == low + 1:
            step(now, low)
        else:

            @pl.loop(low, high)
            def _(it, now=now):
                step(now, it)

        low = high

    energy_copy = remote(energy.at[c], energy.at[c], e_send, e_recv, core_peer)
    energy_copy.start()
    load_groups.wait()
    load_owners.wait()
    for n in range(n_dp - 1):
        magnitude_copy(n).wait_recv()
        if extra:
            share_copy(n).wait_recv()
    mag = magnitude[0]
    for k in range(1, n_dp):
        mag = mag + magnitude[k]
    mag = mag / tok_ref.shape[1]
    if n_tensor > 1:
        pl.semaphore_wait(seen.at[n_tensor - 2], planes)
    tokens = block * n_dp
    if extra:
        both = shared[0]
        for k in range(1, n_dp):
            both = both + shared[k]
        shares = jnp.sqrt(both[:extra] / tokens) * mag[quads : quads + extra]
        shares = jnp.where(chip == 0, shares, 0.0)
    energy_copy.wait()
    score[...] = jnp.sqrt((energy[0] + energy[1]) / tokens) * mag

    lines = lax.broadcasted_iota(jnp.int32, (totals.shape[2], LANES), 0)
    acc = jnp.zeros(lines.shape, jnp.float32)
    for u in range(quads):
        acc = acc + jnp.where(lines == group_buf[pl.ds(ROLES * u + chip, 1), :], score[u : u + 1, :], 0.0)
    for e in range(extra):
        acc = acc + jnp.where(lines == group_buf[items + e : items + e + 1, :], shares[e : e + 1], 0.0)
    slot = ROLES * z + chip
    totals[slot] = jnp.sum(acc.T, axis=0, keepdims=True)
    t_copies = []
    for dz in range(n_tensor):
        for k in range(4):
            if dz or k:
                n = len(t_copies)
                copy = remote(
                    totals.at[slot],
                    totals.at[slot],
                    t_send.at[n],
                    t_recv.at[n],
                    device_at(k % 2, k // 2, True),
                    (z + dz) % n_tensor,
                )
                copy.start()
                t_copies.append(copy)

    for r in range(4):
        for same in (False, True):
            if (r, same) != (0, True):
                token_copy(r, same).wait_send()
        if split(r):
            for copy in plane_copies(r):
                copy.wait_send()
    for n in range(n_dp - 1):
        magnitude_copy(n).wait_send()
        if extra:
            share_copy(n).wait_send()

    @pl.loop(0, items)
    def _(j):
        core_copy(j).wait_send()
        first_copy(j, j).wait_send()
        second_copy(j, j).wait_send()

    for e in range(extra):
        for r in range(4):
            core_x_copy(r, e).wait_send()
        for half in range(2):
            first_x_copy(half, e).wait_send()
        second_x_copy(e).wait_send()

    for copy in t_copies:
        copy.wait()
    row = totals[0]
    for k in range(1, ROLES * n_tensor):
        row = row + totals[k]
    row = row[:, : out_ref.shape[1]] / GROUP
    out_ref[...] = jnp.where(owner_buf[...] == z, row, 0.0)


def fused_shards(n_dp, n_tensor, tokens, gate_weight, up_weight, down_weight, channel_group, owners):
    block = tokens.shape[0]
    depth, width = gate_weight.shape
    chunks = width // LANES
    quads, extra = chunks // ROLES, chunks % ROLES
    items, spare = 4 * quads, max(extra, 1)
    count = owners.shape[0]
    span = down_weight.shape[1]
    lines = -(-(quads + extra) // 8) * 8
    padded = -(-count // LANES) * LANES
    peers = n_dp - 1
    far = max(4 * n_tensor - 1, 1)
    vmem = pl.BlockSpec(memory_space=pltpu.VMEM)
    hbm = pl.BlockSpec(memory_space=pl.ANY)
    dma = pltpu.SemaphoreType.DMA
    tile = (block, 2 * LANES)
    half = jnp.bfloat16
    return pl.pallas_call(
        functools.partial(kernel, n_tensor),
        out_shape=jax.ShapeDtypeStruct((1, count), jnp.float32),
        in_specs=[hbm, hbm, hbm, hbm, hbm, hbm],
        out_specs=vmem,
        scratch_shapes=[
            pltpu.VMEM(tokens.shape, half),
            pltpu.VMEM((4, 2 * block, depth), half),
            pltpu.VMEM((chunks, depth, 2 * LANES), half),
            pltpu.VMEM((chunks, LANES, span), half),
            pltpu.VMEM((chunks, LANES), jnp.int32),
            pltpu.VMEM((1, count), jnp.int32),
            pltpu.VMEM((items, ROLES) + tile, half),
            pltpu.VMEM((items, ROLES) + tile, half),
            pltpu.VMEM((items, ROLES) + tile, half),
            pltpu.VMEM((items, 2) + tile, half),
            pltpu.VMEM((items,) + tile, half),
            pltpu.VMEM((4 * spare,) + tile, half),
            pltpu.VMEM((4 * spare,) + tile, half),
            pltpu.VMEM((4 * spare,) + tile, half),
            pltpu.VMEM((2 * spare,) + tile, half),
            pltpu.VMEM((spare,) + tile, half),
            pltpu.VMEM((2, lines, LANES), jnp.float32),
            pltpu.VMEM((n_dp, 8, LANES), jnp.float32),
            pltpu.VMEM((ROLES, lines, LANES), jnp.float32),
            pltpu.VMEM((n_dp, lines, LANES), jnp.float32),
            pltpu.VMEM((lines, LANES), jnp.float32),
            pltpu.VMEM((ROLES * n_tensor, 1, padded), jnp.float32),
            dma((3,)),
            dma((peers,)),
            dma((chunks,)),
            dma((chunks,)),
            dma((chunks,)),
            dma((n_dp,)),
            dma((n_dp,)),
            dma((items,)),
            dma((items,)),
            dma((items,)),
            dma((items,)),
            dma((items,)),
            dma((items,)),
            dma((4 * spare,)),
            dma((4 * spare,)),
            dma((2 * spare,)),
            dma((2 * spare,)),
            dma((spare,)),
            dma((spare,)),
            dma((peers,)),
            dma((peers,)),
            dma((peers,)),
            dma((peers,)),
            dma,
            dma,
            dma((far,)),
            dma((far,)),
            dma((n_dp * n_tensor,)),
            dma((n_dp * n_tensor,)),
            pltpu.SemaphoreType.REGULAR((max(n_tensor - 1, 1),)),
            pltpu.SemaphoreType.REGULAR((max(n_tensor - 2, 1),)),
        ],
        compiler_params=pltpu.CompilerParams(
            collective_id=0, has_side_effects=True, vmem_limit_bytes=56 * 1024 * 1024
        ),
    )(tokens, gate_weight, up_weight, down_weight, channel_group.reshape(chunks, LANES), owners.reshape(1, count))


def solution(mesh):
    n_dp, n_tensor = mesh.shape["dp"], mesh.shape["tensor"]

    def shards(tokens, gate_weight, *rest):
        if n_dp == 8 and gate_weight.shape[1] % LANES == 0 and gate_weight.shape[1] >= ROLES * LANES:
            return fused_shards(n_dp, n_tensor, tokens, gate_weight, *rest)
        return plain_shards(tokens, gate_weight, *rest)

    return jax.shard_map(
        shards,
        mesh=mesh,
        in_specs=(
            P("dp", None),
            P("dp", "tensor"),
            P("dp", "tensor"),
            P("tensor", "dp"),
            P("tensor"),
            P(),
        ),
        out_specs=P("tensor", None),
        check_vma=False,
    )
```

```python
import functools

import jax
import jax.numpy as jnp
from jax import lax
from jax.experimental import pallas as pl
from jax.experimental.pallas import tpu as pltpu
from jax.sharding import PartitionSpec as P

GROUP = 128
LANES = 128
ROLES = 4
LAG_CORE = 2
LAG_FIRST = 7
HOLD = 0
LAG_SECOND = 3
MAGNITUDE_ROW = 2
SPLIT = (2, 3)
SHARE_SECOND = 4
SHARE_LAST = 5
MESH = pl.DeviceIdType.MESH


def group_sum(channel_score, groups, count):
    onehot = (groups[:, None] == jnp.arange(count, dtype=jnp.int32)[None, :]).astype(jnp.float32)
    return jnp.dot(channel_score, onehot, precision=lax.Precision.HIGHEST) / GROUP


def plain_shards(tokens, gate_weight, up_weight, down_weight, channel_group, owners):
    total_tokens = tokens.shape[0] * lax.axis_size("dp")
    width = gate_weight.shape[1]
    group_count = owners.shape[0]
    magnitude = jnp.sum(jnp.abs(down_weight.astype(jnp.float32)), axis=1) / tokens.shape[1]
    columns = lax.all_to_all(tokens, "dp", split_axis=1, concat_axis=0, tiled=True)
    mixed = lax.psum_scatter(
        jnp.concatenate(
            (
                jnp.dot(columns, gate_weight, preferred_element_type=jnp.float32),
                jnp.dot(columns, up_weight, preferred_element_type=jnp.float32),
            ),
            axis=1,
        ).astype(jnp.bfloat16),
        "dp",
        scatter_dimension=0,
        tiled=True,
    ).astype(jnp.float32)
    hidden = jax.nn.silu(mixed[:, :width]) * mixed[:, width:]
    energy = jnp.sum(hidden * hidden, axis=0) / total_tokens
    energy, magnitude = lax.psum((energy, magnitude), "dp")
    partial_value = group_sum(jnp.sqrt(energy) * magnitude, channel_group, group_count)
    totals = lax.psum(partial_value, "tensor")
    rank = lax.axis_index("tensor")
    row = jnp.where(owners == rank, totals, jnp.float32(0.0))
    return row[None, :]


def kernel(
    n_tensor,
    tok_ref,
    gate_ref,
    up_ref,
    down_ref,
    group_ref,
    owner_ref,
    out_ref,
    tok_buf,
    x_buf,
    w_buf,
    d_buf,
    group_buf,
    owner_buf,
    give,
    keep,
    got_core,
    got_first,
    got_second,
    give_x,
    keep_x,
    got_core_x,
    got_first_x,
    got_second_x,
    energy,
    shared,
    mag_out,
    magnitude,
    score,
    totals,
    local_sem,
    tok_sem,
    w_sem,
    x_send,
    x_recv,
    core_send,
    core_recv,
    first_send,
    first_recv,
    second_send,
    second_recv,
    core_x_send,
    core_x_recv,
    first_x_send,
    first_x_recv,
    second_x_send,
    second_x_recv,
    m_send,
    m_recv,
    s_send,
    s_recv,
    e_send,
    e_recv,
    t_send,
    t_recv,
    z_send,
    z_recv,
    seen,
    met,
):
    n_dp = 8
    chunks = w_buf.shape[0]
    quads, extra = chunks // ROLES, chunks % ROLES
    items = 4 * quads
    block = tok_ref.shape[0]
    depth = x_buf.shape[2]
    me = lax.axis_index("dp")
    z = lax.axis_index("tensor")
    c, x, y = me % 2, (me // 2) % 2, me // 4
    chip = me // 2

    def chip_at(f, s):
        fx, fy = f * (1 - c) + s * c, f * c + s * (1 - c)
        return 2 * (y + fy * (1 - 2 * y)) + x + fx * (1 - 2 * x)

    def device_at(f, s, same):
        return 2 * chip_at(f, s) + (c if same else 1 - c)

    core_peer = device_at(0, 0, False)
    first_peer = device_at(1, 0, True)
    second_peer = device_at(0, 1, True)
    others = [(r % 2, r // 2, same) for r in range(4) for same in (False, True) if (r, same) != (0, True)]

    def remote(src, dst, send, recv, peer, plane=z):
        return pltpu.make_async_remote_copy(
            src_ref=src, dst_ref=dst, send_sem=send, recv_sem=recv, device_id=(peer, plane), device_id_type=MESH
        )

    barrier = pltpu.get_barrier_semaphore()
    near = [hop for hop in others if hop[0] + hop[1] < 2]
    for hop in near:
        pl.semaphore_signal(barrier, inc=1, device_id=(device_at(*hop), z), device_id_type=MESH)

    def signal_planes(sem):
        @pl.when(z > 0)
        def _():
            pl.semaphore_signal(sem, inc=1, device_id=(me, z - 1), device_id_type=MESH)

        @pl.when(z < n_tensor - 1)
        def _():
            pl.semaphore_signal(sem, inc=1, device_id=(me, z + 1), device_id_type=MESH)

    planes = jnp.where(z > 0, 1, 0) + jnp.where(z < n_tensor - 1, 1, 0)
    signal_planes(barrier)

    load_groups = pltpu.make_async_copy(group_ref, group_buf, local_sem.at[0])
    load_owners = pltpu.make_async_copy(owner_ref, owner_buf, local_sem.at[1])
    piece = block // n_tensor

    def split(r):
        return r in SPLIT and n_tensor > 1 and block % (16 * n_tensor) == 0

    def token_rows(r, start):
        if split(r):
            return pl.ds(pl.multiple_of(start + z * piece, piece), piece)
        return pl.ds(start, block)

    def token_columns(f, s, same):
        return pl.ds(pl.multiple_of(device_at(f, s, same) * depth, depth), depth)

    def token_load(n):
        f, s, same = others[n]
        data = (token_rows(f + 2 * s, 0), token_columns(f, s, same))
        return pltpu.make_async_copy(tok_ref.at[data], tok_buf.at[data], tok_sem.at[n])

    load_own = pltpu.make_async_copy(
        tok_ref.at[:, token_columns(0, 0, True)], x_buf.at[0, pl.ds(block, block), :], local_sem.at[2]
    )
    load_own.start()
    for n in range(3):
        token_load(n).start()

    def gate_copy(i):
        cols = pl.ds(pl.multiple_of(i * LANES, LANES), LANES)
        return pltpu.make_async_copy(gate_ref.at[:, cols], w_buf.at[i, :, pl.ds(0, LANES)], w_sem.at[i // ROLES])

    def up_copy(i):
        cols = pl.ds(pl.multiple_of(i * LANES, LANES), LANES)
        return pltpu.make_async_copy(up_ref.at[:, cols], w_buf.at[i, :, pl.ds(LANES, LANES)], w_sem.at[i // ROLES])

    def wait_weights(u, count):
        data = w_buf.at[pl.ds(ROLES * u, count)]
        pltpu.make_async_copy(data, data, w_sem.at[u]).wait()

    load_down = pltpu.make_async_copy(down_ref, d_buf, local_sem.at[3])

    for i in range(ROLES):
        gate_copy(i).start()
        up_copy(i).start()
    for n in range(3, len(others)):
        token_load(n).start()

    @pl.loop(ROLES, chunks)
    def _(i):
        gate_copy(i).start()
        up_copy(i).start()

    def token_copy(r, same):
        cols = token_columns(r % 2, r // 2, same)
        slot = 2 * r + (1 if same else 0)
        start = block if same else 0
        return remote(
            tok_buf.at[token_rows(r, 0), cols],
            x_buf.at[r, token_rows(r, start), :],
            x_send.at[slot],
            x_recv.at[slot],
            device_at(r % 2, r // 2, same),
        )

    def plane_copies(r):
        copies = []
        for same in (False, True):
            data = x_buf.at[r, token_rows(r, block if same else 0), :]
            for dz in range(1, n_tensor):
                copies.append(remote(data, data, z_send.at[r], z_recv.at[r], me, (z + dz) % n_tensor))
        return copies

    def plane_rows(r):
        data = x_buf.at[r, pl.ds(0, 2 * (n_tensor - 1) * piece), :]
        return remote(data, data, z_send.at[r], z_recv.at[r], me)

    sends = [(f + 2 * s, same) for f, s, same in others]
    token_load(0).wait()
    pl.semaphore_wait(barrier, len(near) + planes)
    token_copy(*sends[0]).start()
    for n in range(1, 5):
        token_load(n).wait()
        token_copy(*sends[n]).start()
    if n_tensor > 2:
        signal_planes(met.at[0])
    load_groups.start()
    load_owners.start()

    load_down.start()
    mag_out[...] = jnp.zeros_like(mag_out)
    energy[...] = jnp.zeros_like(energy)
    shared[...] = jnp.zeros_like(shared)
    ones = jnp.ones((8, d_buf.shape[1]), jnp.bfloat16)

    def core_copy(j):
        return remote(give.at[j], got_core.at[j], core_send, core_recv.at[j], core_peer)

    def first_copy(r, u):
        to, sem = got_first.at[r + 1 - 2 * (r % 2), u], first_recv.at[r // 2, u]
        return remote(keep.at[r * quads + u, pl.ds(2, 2)], to, first_send, sem, first_peer)

    def second_copy(r, u):
        to, sem = got_second.at[(r + 2) % 4, u], second_recv.at[(r + 2) % 4 // 2, u]
        return remote(keep.at[r * quads + u, 1], to, second_send, sem, second_peer)

    def wait_first(half, u):
        data = got_first.at[pl.ds(2 * half, 2), u]
        remote(data, data, first_send, first_recv.at[half, u], first_peer).wait_recv()

    def wait_second(half, u):
        data = got_second.at[pl.ds(2 * half, 2), u]
        remote(data, data, second_send, second_recv.at[half, u], second_peer).wait_recv()

    def core_x_copy(r, e):
        j = r * extra + e
        return remote(give_x.at[j], got_core_x.at[j], core_x_send.at[j], core_x_recv.at[j], core_peer)

    def first_x_copy(half, e):
        j = half * extra + e
        source = (2 * half + 1) * extra + e
        return remote(keep_x.at[source], got_first_x.at[j], first_x_send.at[j], first_x_recv.at[j], first_peer)

    def second_x_copy(e):
        return remote(
            keep_x.at[2 * extra + e], got_second_x.at[e], second_x_send.at[e], second_x_recv.at[e], second_peer
        )

    def share_copy(n):
        return remote(shared.at[me], shared.at[me], s_send, s_recv, device_at(*others[n]))

    def magnitude_copy(n):
        f, s, same = others[n]
        return remote(mag_out.at[chip_at(f, s)], magnitude.at[me], m_send, m_recv, device_at(f, s, same))

    def total(*refs):
        value = refs[0].astype(jnp.float32)
        for ref in refs[1:]:
            value = value + ref.astype(jnp.float32)
        return value

    def squares(mixed):
        gate, up = mixed[:, :LANES], mixed[:, LANES:]
        hidden = gate / (1.0 + jnp.exp(-gate)) * up
        return jnp.sum(hidden * hidden, axis=0, keepdims=True)

    swap = (0, 2, 1, 3)
    role_chips = [chip_at(role // 2, role % 2) for role in range(ROLES)]

    def multiply(r, u, j):
        for role in (2, 3, 1, 0):
            product = jnp.dot(
                x_buf[r], w_buf[ROLES * u + role_chips[role]], preferred_element_type=jnp.float32
            ).astype(jnp.bfloat16)
            give[j, swap[role]] = product[:block]
            keep[j, role] = product[block:]

    def fold(half, u):
        wait_first(half, u)
        for r in (2 * half, 2 * half + 1):
            j = r * quads + u
            keep[j, 1] = total(keep[j, 1], got_core[j, 1], got_first[r, u, 1]).astype(jnp.bfloat16)

    def finish(half, u):
        wait_second(half, u)
        parts = []
        for r in (2 * half, 2 * half + 1):
            j = r * quads + u
            parts.append(squares(total(keep[j, 0], got_core[j, 0], got_first[r, u, 0], got_second[r, u])))
        return parts[0] + parts[1]

    fold_starts = (quads + LAG_FIRST + HOLD, 3 * quads + LAG_FIRST)
    final_start = fold_starts[1] + LAG_SECOND
    steps = final_start + quads
    magnitude_start = MAGNITUDE_ROW * quads

    def row_at(it, lag):
        return (it - lag) // quads if 0 <= it - lag < items else None

    def stages(it):
        return (
            row_at(it, 0),
            row_at(it, LAG_CORE),
            tuple(0 <= it - start < quads for start in fold_starts),
            0 <= it - magnitude_start < quads,
            0 <= it - final_start < quads,
        )

    def step(now, it):
        row, core_row, folding, weighing, ending = now
        after_core = it - LAG_CORE
        if core_row is not None:
            core_copy(after_core).wait_recv()
            keep[after_core, 2:] = total(keep[after_core, 2:], got_core[after_core, 2:]).astype(jnp.bfloat16)
        if row is not None:
            u = it - row * quads
            if row == 0:
                wait_weights(u, ROLES)
            multiply(row, u, it)
        if core_row is not None:
            first_copy(core_row, after_core - core_row * quads).start()
        if row is not None:
            core_copy(it).start()
        for half in range(2):
            if folding[half]:
                fold(half, it - fold_starts[half])
        if weighing:
            v = it - magnitude_start
            rows = jnp.abs(d_buf[pl.ds(pl.multiple_of(ROLES * LANES * v, LANES), ROLES * LANES), :])
            sums = lax.dot_general(ones, rows, (((1,), (1,)), ((), ())), preferred_element_type=jnp.float32)
            for k in range(ROLES):
                mag_out[k, pl.ds(v, 1), :] = sums[0:1, k * LANES : (k + 1) * LANES]
        for half in range(2):
            if folding[half]:
                for r in (2 * half, 2 * half + 1):
                    second_copy(r, it - fold_starts[half]).start()
        if folding[1]:
            u = it - fold_starts[1]
            energy[c, pl.ds(u, 1), :] = finish(1, u)
        if ending:
            u = it - final_start
            energy[c, pl.ds(u, 1), :] = energy[c, pl.ds(u, 1), :] + finish(0, u)

    events = {}

    def at(it):
        return lambda run: events.setdefault(it, []).append(run)

    @at(quads)
    def _():
        for same in (True, False):
            token_copy(1, same).wait_recv()
        for n in range(5, 7):
            token_load(n).wait()
            token_copy(*sends[n]).start()

    for n in range(n_tensor - 2):

        @at(1 + n)
        def _(n=n):
            pl.semaphore_wait(met.at[n], planes)
            if n < n_tensor - 3:
                signal_planes(met.at[n + 1])

    for k, when in ((2, min(SHARE_SECOND, 2 * quads)), (3, min(quads + SHARE_LAST, 3 * quads))):
        if split(k):

            @at(when)
            def _(k=k):
                for same in (True, False):
                    token_copy(k, same).wait_recv()
                for copy in plane_copies(k):
                    copy.start()

    for k in (2, 3):

        @at(k * quads)
        def _(k=k):
            for copy in [plane_rows(k)] if split(k) else [token_copy(k, same) for same in (True, False)]:
                copy.wait_recv()

    for n in range(n_tensor - 1):

        @at(quads + 2 + 4 * n)
        def _(n=n):
            if n > 0:
                pl.semaphore_wait(seen.at[n - 1], planes)
            signal_planes(seen.at[n])

    for e in range(extra):
        for r in range(4):
            when = r * quads if r else quads - 1

            @at(when)
            def _(r=r, e=e):
                if r == 0 and e == 0:
                    wait_weights(quads, extra)
                product = jnp.dot(x_buf[r], w_buf[items + e], preferred_element_type=jnp.float32).astype(jnp.bfloat16)
                give_x[r * extra + e] = product[:block]
                keep_x[r * extra + e] = product[block:]
                core_x_copy(r, e).start()

            @at(when + LAG_CORE)
            def _(r=r, e=e):
                core_x_copy(r, e).wait_recv()
                j = r * extra + e
                if r % 2:
                    keep_x[j] = total(keep_x[j], got_core_x[j]).astype(jnp.bfloat16)
                    first_x_copy(r // 2, e).start()

        @at(fold_starts[1])
        def _(e=e):
            first_x_copy(1, e).wait_recv()
            j = 2 * extra + e
            keep_x[j] = total(keep_x[j], got_core_x[j], got_first_x[extra + e]).astype(jnp.bfloat16)
            second_x_copy(e).start()

        @at(magnitude_start + quads)
        def _(e=e):
            rows = jnp.abs(d_buf[(items + e) * LANES : (items + e + 1) * LANES, :])
            sums = lax.dot_general(ones, rows, (((1,), (1,)), ((), ())), preferred_element_type=jnp.float32)
            for k in range(ROLES):
                mag_out[k, quads + e : quads + e + 1, :] = sums[0:1, :]

        @at(fold_starts[1] + quads - 1)
        def _(e=e):
            first_x_copy(0, e).wait_recv()
            second_x_copy(e).wait_recv()
            shared[me, e : e + 1, :] = squares(total(keep_x[e], got_core_x[e], got_first_x[e], got_second_x[e]))

    @at(magnitude_start + quads + 1)
    def _():
        for n in range(n_dp - 1):
            magnitude_copy(n).start()
        magnitude[me] = mag_out[chip]

    if extra:

        @at(fold_starts[1] + quads)
        def _():
            for n in range(n_dp - 1):
                share_copy(n).start()

    at(magnitude_start)(load_down.wait)
    load_own.wait()
    token_copy(0, False).wait_recv()
    low = 0
    while low < steps:
        for run in events.pop(low, ()):
            run()
        now, high = stages(low), low + 1
        while high < steps and stages(high) == now and high not in events:
            high += 1
        if high == low + 1:
            step(now, low)
        else:

            @pl.loop(low, high)
            def _(it, now=now):
                step(now, it)

        low = high

    energy_copy = remote(energy.at[c], energy.at[c], e_send, e_recv, core_peer)
    energy_copy.start()
    load_groups.wait()
    load_owners.wait()
    all_magnitudes = magnitude.at[pl.ds(0, n_dp - 1)]
    magnitudes = remote(all_magnitudes, all_magnitudes, m_send, m_recv, core_peer)
    magnitudes.wait_recv()
    all_shares = shared.at[pl.ds(0, n_dp - 1)]
    shares_in = remote(all_shares, all_shares, s_send, s_recv, core_peer)
    if extra:
        shares_in.wait_recv()
    mag = magnitude[0]
    for k in range(1, n_dp):
        mag = mag + magnitude[k]
    mag = mag / tok_ref.shape[1]
    if n_tensor > 1:
        pl.semaphore_wait(seen.at[n_tensor - 2], planes)
    tokens = block * n_dp
    if extra:
        both = shared[0]
        for k in range(1, n_dp):
            both = both + shared[k]
        shares = jnp.sqrt(both[:extra] / tokens) * mag[quads : quads + extra]
        shares = jnp.where(chip == 0, shares, 0.0)
    energy_copy.wait()
    score[...] = jnp.sqrt((energy[0] + energy[1]) / tokens) * mag

    lines = lax.broadcasted_iota(jnp.int32, (totals.shape[2], LANES), 0)
    acc = jnp.zeros(lines.shape, jnp.float32)
    for u in range(quads):
        acc = acc + jnp.where(lines == group_buf[pl.ds(ROLES * u + chip, 1), :], score[u : u + 1, :], 0.0)
    for e in range(extra):
        acc = acc + jnp.where(lines == group_buf[items + e : items + e + 1, :], shares[e : e + 1], 0.0)
    slot = ROLES * z + chip
    totals[slot] = jnp.sum(acc.T, axis=0, keepdims=True)
    for dz in range(n_tensor):
        for k in range(4):
            if dz or k:
                remote(
                    totals.at[slot],
                    totals.at[slot],
                    t_send,
                    t_recv,
                    device_at(k % 2, k // 2, True),
                    (z + dz) % n_tensor,
                ).start()

    for send in sends:
        token_copy(*send).wait_send()
    for k in SPLIT:
        if split(k):
            plane_rows(k).wait_send()
    magnitudes.wait_send()
    if extra:
        shares_in.wait_send()
    remote(give, give, core_send, core_recv.at[0], core_peer).wait_send()
    first_part = keep.at[:, pl.ds(2, 2)]
    remote(first_part, first_part, first_send, core_recv.at[0], core_peer).wait_send()
    second_part = keep.at[:, 1]
    remote(second_part, second_part, second_send, core_recv.at[0], core_peer).wait_send()
    for e in range(extra):
        for r in range(4):
            core_x_copy(r, e).wait_send()
        for half in range(2):
            first_x_copy(half, e).wait_send()
        second_x_copy(e).wait_send()

    far = ROLES * n_tensor - 1
    all_totals = totals.at[pl.ds(0, far)]
    arrived = remote(all_totals, all_totals, t_send, t_recv, core_peer)
    arrived.wait()
    row = totals[0]
    for k in range(1, ROLES * n_tensor):
        row = row + totals[k]
    row = row[:, : out_ref.shape[1]] / GROUP
    out_ref[...] = jnp.where(owner_buf[...] == z, row, 0.0)


def fused_shards(n_dp, n_tensor, tokens, gate_weight, up_weight, down_weight, channel_group, owners):
    block = tokens.shape[0]
    depth, width = gate_weight.shape
    chunks = width // LANES
    quads, extra = chunks // ROLES, chunks % ROLES
    items, spare = 4 * quads, max(extra, 1)
    count = owners.shape[0]
    span = down_weight.shape[1]
    lines = -(-(quads + extra) // 8) * 8
    padded = -(-count // LANES) * LANES
    peers = n_dp - 1
    vmem = pl.BlockSpec(memory_space=pltpu.VMEM)
    hbm = pl.BlockSpec(memory_space=pl.ANY)
    dma = pltpu.SemaphoreType.DMA
    tile = (block, 2 * LANES)
    half = jnp.bfloat16
    return pl.pallas_call(
        functools.partial(kernel, n_tensor),
        out_shape=jax.ShapeDtypeStruct((1, count), jnp.float32),
        in_specs=[hbm, hbm, hbm, hbm, hbm, hbm],
        out_specs=vmem,
        scratch_shapes=[
            pltpu.VMEM(tokens.shape, half),
            pltpu.VMEM((4, 2 * block, depth), half),
            pltpu.VMEM((chunks, depth, 2 * LANES), half),
            pltpu.VMEM((width, span), half),
            pltpu.VMEM((chunks, LANES), jnp.int32),
            pltpu.VMEM((1, count), jnp.int32),
            pltpu.VMEM((items, ROLES) + tile, half),
            pltpu.VMEM((items, ROLES) + tile, half),
            pltpu.VMEM((items, ROLES) + tile, half),
            pltpu.VMEM((4, quads, 2) + tile, half),
            pltpu.VMEM((4, quads) + tile, half),
            pltpu.VMEM((4 * spare,) + tile, half),
            pltpu.VMEM((4 * spare,) + tile, half),
            pltpu.VMEM((4 * spare,) + tile, half),
            pltpu.VMEM((2 * spare,) + tile, half),
            pltpu.VMEM((spare,) + tile, half),
            pltpu.VMEM((2, lines, LANES), jnp.float32),
            pltpu.VMEM((n_dp, 8, LANES), jnp.float32),
            pltpu.VMEM((ROLES, lines, LANES), jnp.float32),
            pltpu.VMEM((n_dp, lines, LANES), jnp.float32),
            pltpu.VMEM((lines, LANES), jnp.float32),
            pltpu.VMEM((ROLES * n_tensor, 1, padded), jnp.float32),
            dma((4,)),
            dma((peers,)),
            dma((quads + 1,)),
            dma((n_dp,)),
            dma((n_dp,)),
            dma,
            dma((items,)),
            dma,
            dma((2, quads)),
            dma,
            dma((2, quads)),
            dma((4 * spare,)),
            dma((4 * spare,)),
            dma((2 * spare,)),
            dma((2 * spare,)),
            dma((spare,)),
            dma((spare,)),
            dma,
            dma,
            dma,
            dma,
            dma,
            dma,
            dma,
            dma,
            dma((4,)),
            dma((4,)),
            pltpu.SemaphoreType.REGULAR((max(n_tensor - 1, 1),)),
            pltpu.SemaphoreType.REGULAR((max(n_tensor - 2, 1),)),
        ],
        compiler_params=pltpu.CompilerParams(
            collective_id=0, has_side_effects=True, vmem_limit_bytes=56 * 1024 * 1024
        ),
    )(tokens, gate_weight, up_weight, down_weight, channel_group.reshape(chunks, LANES), owners.reshape(1, count))


def solution(mesh):
    n_dp, n_tensor = mesh.shape["dp"], mesh.shape["tensor"]

    def shards(tokens, gate_weight, *rest):
        if n_dp == 8 and gate_weight.shape[1] % LANES == 0 and gate_weight.shape[1] >= ROLES * LANES:
            return fused_shards(n_dp, n_tensor, tokens, gate_weight, *rest)
        return plain_shards(tokens, gate_weight, *rest)

    return jax.shard_map(
        shards,
        mesh=mesh,
        in_specs=(
            P("dp", None),
            P("dp", "tensor"),
            P("dp", "tensor"),
            P("tensor", "dp"),
            P("tensor"),
            P(),
        ),
        out_specs=P("tensor", None),
        check_vma=False,
    )
```

```python
import functools

import jax
import jax.numpy as jnp
from jax import lax
from jax.experimental import pallas as pl
from jax.experimental.pallas import tpu as pltpu
from jax.sharding import PartitionSpec as P

GROUP = 128
LANES = 128
ROLES = 4
LAG_CORE = 2
LAG_FIRST = 7
HOLD = 0
LAG_SECOND = 3
MAGNITUDE_ROW = 2
SPLIT = (2, 3)
SHARE_SECOND = 4
SHARE_LAST = 5
MESH = pl.DeviceIdType.MESH


def group_sum(channel_score, groups, count):
    onehot = (groups[:, None] == jnp.arange(count, dtype=jnp.int32)[None, :]).astype(jnp.float32)
    return jnp.dot(channel_score, onehot, precision=lax.Precision.HIGHEST) / GROUP


def plain_shards(tokens, gate_weight, up_weight, down_weight, channel_group, owners):
    total_tokens = tokens.shape[0] * lax.axis_size("dp")
    width = gate_weight.shape[1]
    group_count = owners.shape[0]
    magnitude = jnp.sum(jnp.abs(down_weight.astype(jnp.float32)), axis=1) / tokens.shape[1]
    columns = lax.all_to_all(tokens, "dp", split_axis=1, concat_axis=0, tiled=True)
    mixed = lax.psum_scatter(
        jnp.concatenate(
            (
                jnp.dot(columns, gate_weight, preferred_element_type=jnp.float32),
                jnp.dot(columns, up_weight, preferred_element_type=jnp.float32),
            ),
            axis=1,
        ).astype(jnp.bfloat16),
        "dp",
        scatter_dimension=0,
        tiled=True,
    ).astype(jnp.float32)
    hidden = jax.nn.silu(mixed[:, :width]) * mixed[:, width:]
    energy = jnp.sum(hidden * hidden, axis=0) / total_tokens
    energy, magnitude = lax.psum((energy, magnitude), "dp")
    partial_value = group_sum(jnp.sqrt(energy) * magnitude, channel_group, group_count)
    totals = lax.psum(partial_value, "tensor")
    rank = lax.axis_index("tensor")
    row = jnp.where(owners == rank, totals, jnp.float32(0.0))
    return row[None, :]


def kernel(
    n_tensor,
    tok_ref,
    gate_ref,
    up_ref,
    down_ref,
    group_ref,
    owner_ref,
    out_ref,
    tok_buf,
    x_buf,
    w_buf,
    d_buf,
    group_buf,
    owner_buf,
    give,
    keep,
    got_core,
    got_first,
    got_second,
    give_x,
    keep_x,
    got_core_x,
    got_first_x,
    got_second_x,
    energy,
    shared,
    mag_out,
    magnitude,
    score,
    totals,
    local_sem,
    tok_sem,
    w_sem,
    x_send,
    x_recv,
    core_send,
    core_recv,
    first_send,
    first_recv,
    second_send,
    second_recv,
    core_x_send,
    core_x_recv,
    first_x_send,
    first_x_recv,
    second_x_send,
    second_x_recv,
    m_send,
    m_recv,
    s_send,
    s_recv,
    e_send,
    e_recv,
    t_send,
    t_recv,
    z_send,
    z_recv,
    seen,
    met,
):
    n_dp = 8
    chunks = w_buf.shape[0]
    quads, extra = chunks // ROLES, chunks % ROLES
    items = 4 * quads
    block = tok_ref.shape[0]
    depth = x_buf.shape[2]
    me = lax.axis_index("dp")
    z = lax.axis_index("tensor")
    c, x, y = me % 2, (me // 2) % 2, me // 4
    chip = me // 2

    def chip_at(f, s):
        fx, fy = f * (1 - c) + s * c, f * c + s * (1 - c)
        return 2 * (y + fy * (1 - 2 * y)) + x + fx * (1 - 2 * x)

    def device_at(f, s, same):
        return 2 * chip_at(f, s) + (c if same else 1 - c)

    core_peer = device_at(0, 0, False)
    first_peer = device_at(1, 0, True)
    second_peer = device_at(0, 1, True)
    others = [(r % 2, r // 2, same) for r in range(4) for same in (False, True) if (r, same) != (0, True)]

    def remote(src, dst, send, recv, peer, plane=z):
        return pltpu.make_async_remote_copy(
            src_ref=src, dst_ref=dst, send_sem=send, recv_sem=recv, device_id=(peer, plane), device_id_type=MESH
        )

    barrier = pltpu.get_barrier_semaphore()
    near = [hop for hop in others if hop[0] + hop[1] < 2]
    for hop in near:
        pl.semaphore_signal(barrier, inc=1, device_id=(device_at(*hop), z), device_id_type=MESH)

    def signal_planes(sem):
        @pl.when(z > 0)
        def _():
            pl.semaphore_signal(sem, inc=1, device_id=(me, z - 1), device_id_type=MESH)

        @pl.when(z < n_tensor - 1)
        def _():
            pl.semaphore_signal(sem, inc=1, device_id=(me, z + 1), device_id_type=MESH)

    planes = jnp.where(z > 0, 1, 0) + jnp.where(z < n_tensor - 1, 1, 0)
    signal_planes(barrier)

    load_groups = pltpu.make_async_copy(group_ref, group_buf, local_sem.at[0])
    load_owners = pltpu.make_async_copy(owner_ref, owner_buf, local_sem.at[1])
    piece = block // n_tensor

    def split(r):
        return r in SPLIT and n_tensor > 1 and block % (16 * n_tensor) == 0

    def token_rows(r, start):
        if split(r):
            return pl.ds(pl.multiple_of(start + z * piece, piece), piece)
        return pl.ds(start, block)

    def token_columns(f, s, same):
        return pl.ds(pl.multiple_of(device_at(f, s, same) * depth, depth), depth)

    def token_load(n):
        f, s, same = others[n]
        data = (token_rows(f + 2 * s, 0), token_columns(f, s, same))
        return pltpu.make_async_copy(tok_ref.at[data], tok_buf.at[data], tok_sem.at[n])

    load_own = pltpu.make_async_copy(
        tok_ref.at[:, token_columns(0, 0, True)], x_buf.at[0, pl.ds(block, block), :], local_sem.at[2]
    )
    load_own.start()
    for n in range(3):
        token_load(n).start()

    def gate_copy(i):
        cols = pl.ds(pl.multiple_of(i * LANES, LANES), LANES)
        return pltpu.make_async_copy(gate_ref.at[:, cols], w_buf.at[i, :, pl.ds(0, LANES)], w_sem.at[i // ROLES])

    def up_copy(i):
        cols = pl.ds(pl.multiple_of(i * LANES, LANES), LANES)
        return pltpu.make_async_copy(up_ref.at[:, cols], w_buf.at[i, :, pl.ds(LANES, LANES)], w_sem.at[i // ROLES])

    def wait_weights(u, count):
        data = w_buf.at[pl.ds(ROLES * u, count)]
        pltpu.make_async_copy(data, data, w_sem.at[u]).wait()

    load_down = pltpu.make_async_copy(down_ref, d_buf, local_sem.at[3])

    for i in range(ROLES):
        gate_copy(i).start()
        up_copy(i).start()
    for n in range(3, len(others)):
        token_load(n).start()

    @pl.loop(ROLES, chunks)
    def _(i):
        gate_copy(i).start()
        up_copy(i).start()

    def token_copy(r, same):
        cols = token_columns(r % 2, r // 2, same)
        start = block if same else 0
        return remote(
            tok_buf.at[token_rows(r, 0), cols],
            x_buf.at[r, token_rows(r, start), :],
            x_send.at[1 if split(r) else 0],
            x_recv.at[r],
            device_at(r % 2, r // 2, same),
        )

    def wait_tokens(r):
        if split(r):
            data = x_buf.at[r, pl.ds(0, 2 * piece), :]
        else:
            data = x_buf.at[r, pl.ds(0, 2 * block if r else block), :]
        remote(data, data, x_send.at[0], x_recv.at[r], core_peer).wait_recv()

    def plane_copies(r):
        copies = []
        for same in (False, True):
            data = x_buf.at[r, token_rows(r, block if same else 0), :]
            for dz in range(1, n_tensor):
                copies.append(remote(data, data, z_send.at[r // 3], z_recv.at[r // 3], me, (z + dz) % n_tensor))
        return copies

    def plane_rows(r):
        data = x_buf.at[r, pl.ds(0, 2 * (n_tensor - 1) * piece), :]
        return remote(data, data, z_send.at[r // 3], z_recv.at[r // 3], core_peer)

    sends = [(f + 2 * s, same) for f, s, same in others]
    token_load(0).wait()
    pl.semaphore_wait(barrier, len(near) + planes)
    token_copy(*sends[0]).start()
    for n in range(1, 5):
        token_load(n).wait()
        token_copy(*sends[n]).start()
    if n_tensor > 2:
        signal_planes(met.at[0])
    load_groups.start()
    load_owners.start()

    load_down.start()
    mag_out[...] = jnp.zeros_like(mag_out)
    energy[...] = jnp.zeros_like(energy)
    shared[...] = jnp.zeros_like(shared)
    ones = jnp.ones((8, d_buf.shape[1]), jnp.bfloat16)

    def core_copy(j):
        return remote(give.at[j], got_core.at[j], core_send, core_recv.at[j], core_peer)

    def first_copy(r, u):
        to, sem = got_first.at[r + 1 - 2 * (r % 2), u], first_recv.at[r // 2, u]
        return remote(keep.at[r * quads + u, pl.ds(2, 2)], to, first_send, sem, first_peer)

    def second_copy(r, u):
        to, sem = got_second.at[(r + 2) % 4, u], second_recv.at[(r + 2) % 4 // 2, u]
        return remote(keep.at[r * quads + u, 1], to, second_send, sem, second_peer)

    def wait_first(half, u):
        data = got_first.at[pl.ds(2 * half, 2), u]
        remote(data, data, first_send, first_recv.at[half, u], first_peer).wait_recv()

    def wait_second(half, u):
        data = got_second.at[pl.ds(2 * half, 2), u]
        remote(data, data, second_send, second_recv.at[half, u], second_peer).wait_recv()

    def core_x_copy(r, e):
        j = r * extra + e
        return remote(give_x.at[j], got_core_x.at[j], core_x_send, core_x_recv.at[j], core_peer)

    def first_x_copy(half, e):
        j = half * extra + e
        source = (2 * half + 1) * extra + e
        return remote(keep_x.at[source], got_first_x.at[j], first_x_send, first_x_recv.at[j], first_peer)

    def second_x_copy(e):
        return remote(
            keep_x.at[2 * extra + e], got_second_x.at[e], second_x_send, second_x_recv.at[e], second_peer
        )

    def share_copy(n):
        return remote(shared.at[me], shared.at[me], s_send, s_recv, device_at(*others[n]))

    def magnitude_copy(n):
        f, s, same = others[n]
        return remote(mag_out.at[chip_at(f, s)], magnitude.at[me], m_send, m_recv, device_at(f, s, same))

    def total(*refs):
        value = refs[0].astype(jnp.float32)
        for ref in refs[1:]:
            value = value + ref.astype(jnp.float32)
        return value

    def squares(mixed):
        gate, up = mixed[:, :LANES], mixed[:, LANES:]
        hidden = gate / (1.0 + jnp.exp(-gate)) * up
        return jnp.sum(hidden * hidden, axis=0, keepdims=True)

    swap = (0, 2, 1, 3)
    role_chips = [chip_at(role // 2, role % 2) for role in range(ROLES)]

    def multiply(r, u, j):
        for role in (2, 3, 1, 0):
            product = jnp.dot(
                x_buf[r], w_buf[ROLES * u + role_chips[role]], preferred_element_type=jnp.float32
            ).astype(jnp.bfloat16)
            give[j, swap[role]] = product[:block]
            keep[j, role] = product[block:]

    def fold(half, u):
        wait_first(half, u)
        for r in (2 * half, 2 * half + 1):
            j = r * quads + u
            keep[j, 1] = total(keep[j, 1], got_core[j, 1], got_first[r, u, 1]).astype(jnp.bfloat16)

    def finish(half, u):
        wait_second(half, u)
        parts = []
        for r in (2 * half, 2 * half + 1):
            j = r * quads + u
            parts.append(squares(total(keep[j, 0], got_core[j, 0], got_first[r, u, 0], got_second[r, u])))
        return parts[0] + parts[1]

    fold_starts = (quads + LAG_FIRST + HOLD, 3 * quads + LAG_FIRST)
    final_start = fold_starts[1] + LAG_SECOND
    steps = final_start + quads
    magnitude_start = MAGNITUDE_ROW * quads

    def row_at(it, lag):
        return (it - lag) // quads if 0 <= it - lag < items else None

    def stages(it):
        return (
            row_at(it, 0),
            row_at(it, LAG_CORE),
            tuple(0 <= it - start < quads for start in fold_starts),
            0 <= it - magnitude_start < quads,
            0 <= it - final_start < quads,
        )

    def step(now, it):
        row, core_row, folding, weighing, ending = now
        after_core = it - LAG_CORE
        if core_row is not None:
            core_copy(after_core).wait_recv()
            keep[after_core, 2:] = total(keep[after_core, 2:], got_core[after_core, 2:]).astype(jnp.bfloat16)
        if row is not None:
            u = it - row * quads
            if row == 0:
                wait_weights(u, ROLES)
            multiply(row, u, it)
        if core_row is not None:
            first_copy(core_row, after_core - core_row * quads).start()
        if row is not None:
            core_copy(it).start()
        for half in range(2):
            if folding[half]:
                fold(half, it - fold_starts[half])
        if weighing:
            v = it - magnitude_start
            rows = jnp.abs(d_buf[pl.ds(pl.multiple_of(ROLES * LANES * v, LANES), ROLES * LANES), :])
            sums = lax.dot_general(ones, rows, (((1,), (1,)), ((), ())), preferred_element_type=jnp.float32)
            for k in range(ROLES):
                mag_out[k, pl.ds(v, 1), :] = sums[0:1, k * LANES : (k + 1) * LANES]
        for half in range(2):
            if folding[half]:
                for r in (2 * half, 2 * half + 1):
                    second_copy(r, it - fold_starts[half]).start()
        if folding[1]:
            u = it - fold_starts[1]
            energy[c, pl.ds(u, 1), :] = finish(1, u)
        if ending:
            u = it - final_start
            energy[c, pl.ds(u, 1), :] = energy[c, pl.ds(u, 1), :] + finish(0, u)

    events = {}

    def at(it):
        return lambda run: events.setdefault(it, []).append(run)

    @at(quads)
    def _():
        wait_tokens(1)
        for n in range(5, 7):
            token_load(n).wait()
            token_copy(*sends[n]).start()

    for n in range(n_tensor - 2):

        @at(1 + n)
        def _(n=n):
            pl.semaphore_wait(met.at[n], planes)
            if n < n_tensor - 3:
                signal_planes(met.at[n + 1])

    for k, when in ((2, min(SHARE_SECOND, 2 * quads)), (3, min(quads + SHARE_LAST, 3 * quads))):
        if split(k):

            @at(when)
            def _(k=k):
                wait_tokens(k)
                for copy in plane_copies(k):
                    copy.start()

    for k in (2, 3):

        @at(k * quads)
        def _(k=k):
            if split(k):
                plane_rows(k).wait_recv()
            else:
                wait_tokens(k)

    for n in range(n_tensor - 1):

        @at(quads + 2 + 4 * n)
        def _(n=n):
            if n > 0:
                pl.semaphore_wait(seen.at[n - 1], planes)
            signal_planes(seen.at[n])

    for e in range(extra):
        for r in range(4):
            when = r * quads if r else quads - 1

            @at(when)
            def _(r=r, e=e):
                if r == 0 and e == 0:
                    wait_weights(quads, extra)
                product = jnp.dot(x_buf[r], w_buf[items + e], preferred_element_type=jnp.float32).astype(jnp.bfloat16)
                give_x[r * extra + e] = product[:block]
                keep_x[r * extra + e] = product[block:]
                core_x_copy(r, e).start()

            @at(when + LAG_CORE)
            def _(r=r, e=e):
                core_x_copy(r, e).wait_recv()
                j = r * extra + e
                if r % 2:
                    keep_x[j] = total(keep_x[j], got_core_x[j]).astype(jnp.bfloat16)
                    first_x_copy(r // 2, e).start()

        @at(fold_starts[1])
        def _(e=e):
            first_x_copy(1, e).wait_recv()
            j = 2 * extra + e
            keep_x[j] = total(keep_x[j], got_core_x[j], got_first_x[extra + e]).astype(jnp.bfloat16)
            second_x_copy(e).start()

        @at(magnitude_start + quads)
        def _(e=e):
            rows = jnp.abs(d_buf[(items + e) * LANES : (items + e + 1) * LANES, :])
            sums = lax.dot_general(ones, rows, (((1,), (1,)), ((), ())), preferred_element_type=jnp.float32)
            for k in range(ROLES):
                mag_out[k, quads + e : quads + e + 1, :] = sums[0:1, :]

        @at(fold_starts[1] + quads - 1)
        def _(e=e):
            first_x_copy(0, e).wait_recv()
            second_x_copy(e).wait_recv()
            shared[me, e : e + 1, :] = squares(total(keep_x[e], got_core_x[e], got_first_x[e], got_second_x[e]))

    @at(magnitude_start + quads + 1)
    def _():
        for n in range(n_dp - 1):
            magnitude_copy(n).start()
        magnitude[me] = mag_out[chip]

    if extra:

        @at(fold_starts[1] + quads)
        def _():
            for n in range(n_dp - 1):
                share_copy(n).start()

    at(magnitude_start)(load_down.wait)
    load_own.wait()
    wait_tokens(0)
    low = 0
    while low < steps:
        for run in events.pop(low, ()):
            run()
        now, high = stages(low), low + 1
        while high < steps and stages(high) == now and high not in events:
            high += 1
        if high == low + 1:
            step(now, low)
        else:

            @pl.loop(low, high)
            def _(it, now=now):
                step(now, it)

        low = high

    energy_copy = remote(energy.at[c], energy.at[c], e_send, e_recv, core_peer)
    energy_copy.start()
    load_groups.wait()
    load_owners.wait()
    all_magnitudes = magnitude.at[pl.ds(0, n_dp - 1)]
    magnitudes = remote(all_magnitudes, all_magnitudes, m_send, m_recv, core_peer)
    magnitudes.wait_recv()
    all_shares = shared.at[pl.ds(0, n_dp - 1)]
    shares_in = remote(all_shares, all_shares, s_send, s_recv, core_peer)
    if extra:
        shares_in.wait_recv()
    mag = magnitude[0]
    for k in range(1, n_dp):
        mag = mag + magnitude[k]
    mag = mag / tok_ref.shape[1]
    if n_tensor > 1:
        pl.semaphore_wait(seen.at[n_tensor - 2], planes)
    tokens = block * n_dp
    if extra:
        both = shared[0]
        for k in range(1, n_dp):
            both = both + shared[k]
        shares = jnp.sqrt(both[:extra] / tokens) * mag[quads : quads + extra]
        shares = jnp.where(chip == 0, shares, 0.0)
    energy_copy.wait()
    score[...] = jnp.sqrt((energy[0] + energy[1]) / tokens) * mag

    lines = lax.broadcasted_iota(jnp.int32, (totals.shape[2], LANES), 0)
    acc = jnp.zeros(lines.shape, jnp.float32)
    for u in range(quads):
        acc = acc + jnp.where(lines == group_buf[pl.ds(ROLES * u + chip, 1), :], score[u : u + 1, :], 0.0)
    for e in range(extra):
        acc = acc + jnp.where(lines == group_buf[items + e : items + e + 1, :], shares[e : e + 1], 0.0)
    slot = ROLES * z + chip
    totals[slot] = jnp.sum(acc.T, axis=0, keepdims=True)
    for dz in range(n_tensor):
        for k in range(4):
            if dz or k:
                remote(
                    totals.at[slot],
                    totals.at[slot],
                    t_send,
                    t_recv,
                    device_at(k % 2, k // 2, True),
                    (z + dz) % n_tensor,
                ).start()

    for cut in (False, True):
        count = sum(split(r) == cut for r, _ in sends)
        if count:
            data = tok_buf.at[pl.ds(0, piece if cut else block), pl.ds(0, count * depth)]
            remote(data, data, x_send.at[1 if cut else 0], x_recv.at[0], core_peer).wait_send()
    for k in SPLIT:
        if split(k):
            plane_rows(k).wait_send()
    magnitudes.wait_send()
    if extra:
        shares_in.wait_send()
    remote(give, give, core_send, core_recv.at[0], core_peer).wait_send()
    first_part = keep.at[:, pl.ds(2, 2)]
    remote(first_part, first_part, first_send, core_recv.at[0], core_peer).wait_send()
    second_part = keep.at[:, 1]
    remote(second_part, second_part, second_send, core_recv.at[0], core_peer).wait_send()
    if extra:
        for ref, sem in ((give_x, core_x_send), (got_first_x, first_x_send), (got_second_x, second_x_send)):
            remote(ref, ref, sem, core_recv.at[0], core_peer).wait_send()

    far = ROLES * n_tensor - 1
    all_totals = totals.at[pl.ds(0, far)]
    arrived = remote(all_totals, all_totals, t_send, t_recv, core_peer)
    arrived.wait()
    row = totals[0]
    for k in range(1, ROLES * n_tensor):
        row = row + totals[k]
    row = row[:, : out_ref.shape[1]] / GROUP
    out_ref[...] = jnp.where(owner_buf[...] == z, row, 0.0)


def fused_shards(n_dp, n_tensor, tokens, gate_weight, up_weight, down_weight, channel_group, owners):
    block = tokens.shape[0]
    depth, width = gate_weight.shape
    chunks = width // LANES
    quads, extra = chunks // ROLES, chunks % ROLES
    items, spare = 4 * quads, max(extra, 1)
    count = owners.shape[0]
    span = down_weight.shape[1]
    lines = -(-(quads + extra) // 8) * 8
    padded = -(-count // LANES) * LANES
    peers = n_dp - 1
    vmem = pl.BlockSpec(memory_space=pltpu.VMEM)
    hbm = pl.BlockSpec(memory_space=pl.ANY)
    dma = pltpu.SemaphoreType.DMA
    tile = (block, 2 * LANES)
    half = jnp.bfloat16
    return pl.pallas_call(
        functools.partial(kernel, n_tensor),
        out_shape=jax.ShapeDtypeStruct((1, count), jnp.float32),
        in_specs=[hbm, hbm, hbm, hbm, hbm, hbm],
        out_specs=vmem,
        scratch_shapes=[
            pltpu.VMEM(tokens.shape, half),
            pltpu.VMEM((4, 2 * block, depth), half),
            pltpu.VMEM((chunks, depth, 2 * LANES), half),
            pltpu.VMEM((width, span), half),
            pltpu.VMEM((chunks, LANES), jnp.int32),
            pltpu.VMEM((1, count), jnp.int32),
            pltpu.VMEM((items, ROLES) + tile, half),
            pltpu.VMEM((items, ROLES) + tile, half),
            pltpu.VMEM((items, ROLES) + tile, half),
            pltpu.VMEM((4, quads, 2) + tile, half),
            pltpu.VMEM((4, quads) + tile, half),
            pltpu.VMEM((4 * spare,) + tile, half),
            pltpu.VMEM((4 * spare,) + tile, half),
            pltpu.VMEM((4 * spare,) + tile, half),
            pltpu.VMEM((2 * spare,) + tile, half),
            pltpu.VMEM((spare,) + tile, half),
            pltpu.VMEM((2, lines, LANES), jnp.float32),
            pltpu.VMEM((n_dp, 8, LANES), jnp.float32),
            pltpu.VMEM((ROLES, lines, LANES), jnp.float32),
            pltpu.VMEM((n_dp, lines, LANES), jnp.float32),
            pltpu.VMEM((lines, LANES), jnp.float32),
            pltpu.VMEM((ROLES * n_tensor, 1, padded), jnp.float32),
            dma((4,)),
            dma((peers,)),
            dma((quads + 1,)),
            dma((2,)),
            dma((4,)),
            dma,
            dma((items,)),
            dma,
            dma((2, quads)),
            dma,
            dma((2, quads)),
            dma,
            dma((4 * spare,)),
            dma,
            dma((2 * spare,)),
            dma,
            dma((spare,)),
            dma,
            dma,
            dma,
            dma,
            dma,
            dma,
            dma,
            dma,
            dma((2,)),
            dma((2,)),
            pltpu.SemaphoreType.REGULAR((max(n_tensor - 1, 1),)),
            pltpu.SemaphoreType.REGULAR((max(n_tensor - 2, 1),)),
        ],
        compiler_params=pltpu.CompilerParams(
            collective_id=0, has_side_effects=True, vmem_limit_bytes=56 * 1024 * 1024
        ),
    )(tokens, gate_weight, up_weight, down_weight, channel_group.reshape(chunks, LANES), owners.reshape(1, count))


def solution(mesh):
    n_dp, n_tensor = mesh.shape["dp"], mesh.shape["tensor"]

    def shards(tokens, gate_weight, *rest):
        if n_dp == 8 and gate_weight.shape[1] % LANES == 0 and gate_weight.shape[1] >= ROLES * LANES:
            return fused_shards(n_dp, n_tensor, tokens, gate_weight, *rest)
        return plain_shards(tokens, gate_weight, *rest)

    return jax.shard_map(
        shards,
        mesh=mesh,
        in_specs=(
            P("dp", None),
            P("dp", "tensor"),
            P("dp", "tensor"),
            P("tensor", "dp"),
            P("tensor"),
            P(),
        ),
        out_specs=P("tensor", None),
        check_vma=False,
    )
```
